256 devices in a mesh: table: 128 (over x, z, y), dp: 2 (over core).
Axes of the slice: x: 4, y: 4, z: 8, core: 2. Of those that a mesh axis runs over, the one named last changes fastest.
Arguments:
- tables: bfloat16 [4, 524288, 128], P(None, 'table'), may hold values from -6 to 6
- owner_ids: int32 [256, 4, 256, 1], P(('table', 'dp')), may hold values from 0 to 127; in each aligned block of 256 rows (0 to 255, 256 to 511, ..., all dimensions but the last counted through in order) at most 4 rows name the same one
- row_ids: int32 [256, 4, 256], P(('table', 'dp')), may hold values from 0 to 4095
- session_of: int32 [256, 256], P(('table', 'dp')), may hold values from 0 to 1, never falling along the last dimension, each value on 1 to 200 neighbouring positions
- relevance: float32 [256, 256], P(('table', 'dp')), may hold values from 0.1 to 10
- logit_bias: float32 [256, 256], P(('table', 'dp')), may hold values from -400 to 400
- w_hidden: float32 [512, 512], replicated, may hold values from -0.25 to 0.25
- bias_hidden: float32 [512], replicated, may hold values from -3 to 3
- w_score: float32 [512], replicated, may hold values from -0.9 to 0.9
Outputs:
- emb_step: float32 [4, 524288, 128], P(None, ('table', 'dp'))
- step_hidden: float32 [512, 512], replicated
- step_bias: float32 [512], replicated
- step_score: float32 [512], replicated
- loss: float32 [], replicated
The draws below stay inside these ranges and needn't reach their ends.
Inputs may be any that keep to these rules, and one draw needn't show every extreme that they name: `owner_ids`: among one device's impressions, for one table, at most 4 name the same owner. `session_of`: session numbers never fall along a device's impressions; each of a device's 2 sessions has 1 to 200 impressions.
All inputs are finite; a program needn't handle non-finite values.
Results may differ from the reference program's by a relative error of at most 0.001.
The reference program's roundings to bfloat16 on the way (of `inputs`, `hidden_bf`, `pre_grad_bf` and `input_grad`) count: a program that leaves them out, or rounds other values in their place, can miss the bound.
Values may be sent and summed in bfloat16 or wider, within the bound.
No kernel may reach another device: no remote copies, remote signals or barrier semaphores. Data moves between devices by JAX's collectives and lax.ppermute only.
A program may use at most 64 MiB of HBM per device.

```python
import math
import jax
import jax.numpy as jnp
import numpy as np
from jax import lax

EMB = 128
ROWS_DEV = 4096
TABLES = 4
HID = 512
SLOTS = 200
SESS_DEV = 2
IMP_DEV = 256
CAP = 4
FEAT = 512
ROWS = 524288
SESSIONS = 512
N_TABLE = 128
DEVICES = 256


def draw_logit_bias(key, part):
    key_base = jax.random.fold_in(jax.random.fold_in(key, 71), 0)
    return jnp.clip(jax.random.normal(key_base, (DEVICES, IMP_DEV), jnp.float32), -6.0, 6.0)


def with_ends(drawn, key, low, largest):
    dims = drawn.shape
    spot = [jax.random.randint(jax.random.fold_in(key, axis), (), 0, dims[axis]) for axis in range(len(dims))]
    drawn = drawn.at[tuple(spot)].set(low)
    longest = dims.index(max(dims))
    spot[longest] = (spot[longest] + 1) % dims[longest]
    return drawn.at[tuple(spot)].set(largest)


def block_levels(stream_key, dims, cuts, low, high):
    factor_of, own = 1.0, jax.random.fold_in(stream_key, 6)
    for axis_at, shards_of in cuts:
        steps = jnp.exp(jax.random.uniform(jax.random.fold_in(own, axis_at), (shards_of,), jnp.float32, low / len(cuts), high / len(cuts)))
        factor_of = factor_of * jnp.repeat(steps, dims[axis_at] // shards_of).reshape([-1 if axis == axis_at else 1 for axis in range(len(dims))])
    return factor_of


def rank_bounds(number_of, lean):
    weights = [(1 << 20) // math.isqrt(grade ** lean) + 1 for grade in range(1, number_of + 1)]
    deviation = 1 + sum(weights) // (1 << 30)
    return np.cumsum(np.array([max(1, weight // deviation) for weight in weights]))


def skewed_ids(rng, shape, count, lean):
    table = rank_bounds(count, lean)
    pick = jax.random.randint(jax.random.fold_in(rng, 1), shape, 0, int(table[count - 1]))
    rank = jnp.searchsorted(jnp.asarray(table, jnp.int32), pick, side="right")
    return jax.random.permutation(jax.random.fold_in(rng, 2), count)[rank].astype(jnp.int32)


def split_up(number_of, total, bound, skew):
    portions = [(1 << 20) // math.isqrt(rank ** skew) + 1 for rank in range(2, number_of + 1)]
    surplus, counts = total - bound - (number_of - 1), [1] * (number_of - 1)
    while surplus > 0:
        movable = [i for i in range(number_of - 1) if counts[i] < bound]
        pool, left = sum([portions[i] for i in movable]), surplus
        for i in movable:
            addition = min(bound - counts[i], max(1, left * portions[i] // pool), surplus)
            counts[i] = counts[i] + addition
            surplus = surplus - addition
    return np.array([bound] + counts)


def ragged(own_key, number_of, total, most, slope):
    if number_of == 2:
        one = jax.random.randint(own_key, (), max(1, total - most), min(most, total - 1) + 1)
        return jnp.stack([one, total - one])
    sizes = jnp.asarray(split_up(number_of, total, most, slope), jnp.int32)
    couples = (number_of - 1) // 2
    donor, receiver = sizes[1:1 + 2 * couples:2], sizes[2:2 + 2 * couples:2]
    room = jnp.minimum(donor - 1, most - receiver)
    moved = jax.random.randint(jax.random.fold_in(own_key, 1), (couples,), 0, 1 << 20) % (room + 1)
    sizes = sizes.at[1:1 + 2 * couples:2].set(donor - moved).at[2:2 + 2 * couples:2].set(receiver + moved)
    return sizes[jax.random.permutation(jax.random.fold_in(own_key, 2), number_of)]


def assign_block(own_key, own, number, rows, count, top, limit, slope):
    ranking = jax.random.permutation(own_key, count)
    heavy_load, usual = portions_of(count, rows * top, limit, slope, True), portions_of(count, rows * top, limit, slope, False)
    places = jnp.arange(count)

    def named(lengths, rotation):
        used = int((lengths > 0).sum())
        fixed = max(1, used // 4)
        moved = fixed + (places - fixed + rotation * (used - fixed)) % max(1, count - fixed)
        return jnp.zeros((count,), jnp.int32).at[ranking[jnp.where(places < fixed, places, moved)]].set(jnp.asarray(lengths, jnp.int32))

    lengths = jnp.where(number % 4 == 0, named(heavy_load, number // 4), named(usual, number - number // 4 - 1))
    mixed = jax.random.permutation(jax.random.fold_in(own, 3), count)
    giver, sink = mixed[0:count // 2 * 2:2], mixed[1:count // 2 * 2:2]
    room = jnp.minimum(lengths[giver] - 1, limit - lengths[sink]) // 2
    room = jnp.where((giver == ranking[0]) | (sink == ranking[0]) | (lengths[sink] == 0), 0, jnp.maximum(room, 0))
    moved = jax.random.randint(jax.random.fold_in(own, 4), (count // 2,), 0, 1 << 20) % (room + 1)
    lengths = lengths.at[giver].add(-moved).at[sink].add(moved)
    labels = jnp.searchsorted(jnp.cumsum(lengths), jnp.arange(rows * top), side="right").astype(jnp.int32)
    grid = labels.reshape(top, rows).T
    grid = grid[jax.random.permutation(jax.random.fold_in(own, 1), rows)]
    rotation = jax.random.randint(jax.random.fold_in(own, 2), (rows, 1), 0, top)
    return jnp.take_along_axis(grid, (jnp.arange(top)[None, :] + rotation) % top, axis=1)


def portions_of(amount, total, reach, slope, full):
    loads = [(1 << 20) // math.isqrt(rank ** slope) + 1 for rank in range(1, amount + 1)]
    largest = reach if full else min(reach, max(-(-total // amount), total * loads[0] // sum(loads)))
    least = 1 if total - largest >= amount - 1 else 0
    counts, surplus = [largest] + [least] * (amount - 1), total - largest - least * (amount - 1)
    while surplus > 0:
        candidates = [i for i in range(1, amount) if counts[i] < largest] or [i for i in range(1, amount) if counts[i] < reach]
        pool, left = sum([loads[i] for i in candidates]), surplus
        for i in candidates:
            more = min(reach - counts[i], max(1, left * loads[i] // pool), surplus)
            counts[i] = counts[i] + more
            surplus = surplus - more
    return np.array(counts)


def normal_values(rng, extent, spread, most, cuts=(), kind=jnp.bfloat16):
    array = jax.random.normal(rng, extent, jnp.float32) * spread
    if len(cuts) > 0:
        array = block_levels(rng, extent, cuts, -0.22, 0.18) * array
    return jnp.clip(array, min=-most, max=most).astype(kind)


def setup_inputs(seed: int = 0) -> dict:
    streams_of = jax.random.split(jax.random.key(seed), 10)
    tables = normal_values(streams_of[0], (TABLES, ROWS, EMB), 1.0, 6.0, ((1, 128),))
    owner_ids_keys = jax.random.split(jax.random.fold_in(streams_of[1], 1), DEVICES * TABLES * IMP_DEV // IMP_DEV)
    owner_ids_turns = jax.random.permutation(jax.random.fold_in(streams_of[1], 3), DEVICES * TABLES * IMP_DEV // IMP_DEV)
    owner_ids = jax.vmap(lambda own, number: assign_block(jax.random.fold_in(streams_of[1], 2), own, number, IMP_DEV, N_TABLE, 1, CAP, 1))(owner_ids_keys, owner_ids_turns).reshape((DEVICES, TABLES, IMP_DEV, 1))
    row_ids = with_ends(skewed_ids(streams_of[2], (DEVICES, TABLES, IMP_DEV), ROWS_DEV, 2), jax.random.fold_in(streams_of[2], 3), 0, ROWS_DEV - 1).astype(jnp.int32)
    session_of = jax.vmap(lambda own: jnp.searchsorted(jnp.cumsum(ragged(own, SESS_DEV, IMP_DEV, SLOTS, 1)), jnp.arange(IMP_DEV), side="right"))(jax.random.split(streams_of[3], DEVICES)).reshape((DEVICES, IMP_DEV)).astype(jnp.int32)
    relevance = jnp.clip(jnp.exp(math.log(10.0) - 4.6051702 * jax.random.uniform(streams_of[4], (DEVICES, IMP_DEV), jnp.float32) ** block_levels(streams_of[4], (DEVICES, IMP_DEV), ((0, 256),), -0.2, 0.2)), 0.1, 10.0)
    logit_bias = draw_logit_bias(jax.random.fold_in(streams_of[9], 71), 0)
    w_hidden = normal_values(streams_of[6], (FEAT, HID), FEAT ** -0.5, 0.25, (), jnp.float32)
    bias_hidden = normal_values(streams_of[7], (HID,), 0.5, 3.0, (), jnp.float32)
    w_score = normal_values(streams_of[8], (HID,), 0.15, 0.9, (), jnp.float32)
    return {"tables": tables, "owner_ids": owner_ids, "row_ids": row_ids, "session_of": session_of, "relevance": relevance, "logit_bias": logit_bias, "w_hidden": w_hidden, "bias_hidden": bias_hidden, "w_score": w_score}


def silu_slope(pre_val):
    logistic = jax.nn.sigmoid(pre_val)
    return logistic * (1.0 + pre_val * (1.0 - logistic))

def session_terms(scores, session_ids, relevance, sessions):
    member = session_ids[None, :] == jnp.arange(sessions, dtype=jnp.int32)[:, None]
    highest = lax.optimization_barrier(jnp.max(jnp.where(member, scores[None, :], -jnp.inf), axis=1))
    highest_each = lax.optimization_barrier(jnp.sum(jnp.where(member, highest[:, None], 0.0), axis=0))
    shifted = scores - highest_each
    exponent = jnp.exp(shifted)
    totals = lax.optimization_barrier(jnp.sum(jnp.where(member, exponent[None, :], 0.0), axis=1))
    weights = lax.optimization_barrier(jnp.sum(jnp.where(member, relevance[None, :], 0.0), axis=1))
    total_each = lax.optimization_barrier(jnp.sum(jnp.where(member, totals[:, None], 0.0), axis=0))
    weight_each = lax.optimization_barrier(jnp.sum(jnp.where(member, weights[:, None], 0.0), axis=0))
    probability = exponent / total_each
    target = relevance / weight_each
    loss_sum = jnp.sum(jnp.log(totals)) - jnp.sum(target * shifted)
    return (loss_sum, probability - target)

def reference(tables, owner_ids, row_ids, session_of, relevance, logit_bias, w_hidden, bias_hidden, w_score):
    hidden_bf = w_hidden.astype(jnp.bfloat16)
    global_rows = owner_ids[:, :, :, 0] * ROWS_DEV + row_ids
    table_index = jnp.arange(TABLES, dtype=jnp.int32)

    def block_step(carry, block):
        weight_acc, bias_acc, score_acc, loss_acc = carry
        rows_here, session_ids, relevant, bias_row = block
        fetched = tables[table_index[None, :], rows_here.T]
        inputs = fetched.reshape(IMP_DEV, TABLES * EMB)
        pre_act = jnp.dot(inputs, hidden_bf, preferred_element_type=jnp.float32) + bias_hidden
        hidden = jax.nn.silu(pre_act)
        scores = jnp.dot(hidden, w_score, precision=lax.Precision.HIGHEST) + bias_row
        loss_sum, score_grad = session_terms(scores, session_ids, relevant, SESS_DEV)
        pre_grad = score_grad[:, None] * w_score[None, :] * silu_slope(pre_act)
        pre_grad_bf = pre_grad.astype(jnp.bfloat16)
        weight_grad = lax.dot_general(inputs, pre_grad_bf, (((0,), (0,)), ((), ())), preferred_element_type=jnp.float32)
        bias_grad = lax.optimization_barrier(jnp.sum(pre_grad, axis=0))
        score_weight_grad = jnp.dot(score_grad, hidden, precision=lax.Precision.HIGHEST)
        input_grad = jnp.dot(pre_grad_bf, hidden_bf.T, preferred_element_type=jnp.float32).astype(jnp.bfloat16)
        carry = (weight_acc + weight_grad, bias_acc + bias_grad, score_acc + score_weight_grad, loss_acc + loss_sum)
        return (carry, input_grad.reshape(IMP_DEV, TABLES, EMB))
    init = (jnp.zeros((FEAT, HID), jnp.float32), jnp.zeros((HID,), jnp.float32), jnp.zeros((HID,), jnp.float32), jnp.zeros((), jnp.float32))
    totals, grads = lax.scan(block_step, init, (global_rows, session_of, relevance, logit_bias))
    weight_tot, bias_tot, score_tot, loss_tot = totals
    row_grad = jnp.zeros((TABLES, ROWS, EMB), jnp.float32)
    row_grad = row_grad.at[table_index[None, None, :], jnp.transpose(global_rows, (0, 2, 1))].add(grads.astype(jnp.float32))
    emb_step = row_grad / (jnp.sqrt(lax.optimization_barrier(jnp.mean(row_grad * row_grad, axis=2, keepdims=True))) + 1e-06)
    param_count = FEAT * HID + 2 * HID
    mean_sq = (jnp.sum(weight_tot * weight_tot) + jnp.sum(bias_tot * bias_tot) + jnp.sum(score_tot * score_tot)) / param_count
    factor = 1.0 / jnp.sqrt(mean_sq + 1e-06)
    loss = loss_tot / SESSIONS
    return (emb_step, weight_tot * factor, bias_tot * factor, score_tot * factor, loss)
```

```python
import jax
import jax.numpy as jnp
from jax import lax
from jax.experimental import pallas as pl
from jax.experimental.pallas import tpu as pltpu
from jax.sharding import Mesh
from jax.sharding import PartitionSpec as P


TABLE = ("x", "z", "y")
ALL = ("x", "z", "y", "dp")
TABLES = 4
CAP = 4
LINES = TABLES * CAP
OWNERS = 128
IMPS = 256
EMB = 128
ROWS = 4096
HID = 512
VMEM = pl.BlockSpec(memory_space=pltpu.VMEM)
ANY = pl.BlockSpec(memory_space=pl.ANY)
BF = jnp.bfloat16
F32 = jnp.float32


def iota(shape, dim):
    return lax.broadcasted_iota(jnp.int32, shape, dim)


def hot_rows(low, block, blocks):
    n = low.shape[0]
    one = jnp.where(iota((n, 128), 1) == low, 1.0, 0.0).astype(BF)
    which = jnp.broadcast_to(block, (n, 128)).astype(F32).astype(BF)
    zero = jnp.zeros((n, 128), BF)
    return jnp.concatenate([jnp.where(which == BF(c), one, zero) for c in range(blocks)], axis=1)


def hot_cols(low, block, blocks):
    n = low.shape[1]
    one = jnp.where(iota((128, n), 0) == low, 1.0, 0.0).astype(BF)
    which = jnp.broadcast_to(block, (128, n)).astype(F32).astype(BF)
    zero = jnp.zeros((128, n), BF)
    return jnp.concatenate([jnp.where(which == BF(c), one, zero) for c in range(blocks)], axis=0)


def slots_kernel(own_ref, row_ref, want_ref, slot_ref, slot_col_ref):
    own = own_ref[...]
    own_rows = [
        jnp.concatenate([own[2 * t : 2 * t + 1], own[2 * t + 1 : 2 * t + 2]], axis=1)
        for t in range(TABLES)
    ]
    own_cols = jnp.transpose(jnp.concatenate(own_rows + own_rows, axis=0))
    row_cols = jnp.transpose(jnp.concatenate([row_ref[...], row_ref[...]], axis=0))
    before = iota((IMPS, IMPS), 0) < iota((IMPS, IMPS), 1)
    slots = []
    for t in range(TABLES):
        same = (own_cols[:, t : t + 1] == own_rows[t]) & before
        rank = jnp.sum(jnp.where(same, 1, 0), axis=0, keepdims=True)
        slots.append(own_rows[t] * LINES + (CAP * t) + rank)
    slot_ref[...] = jnp.concatenate(slots, axis=0)
    slot_cols = jnp.transpose(jnp.concatenate(slots + slots, axis=0))
    slot_col_ref[...] = slot_cols
    lines = []
    for t in range(TABLES):
        slot = jnp.broadcast_to(slot_cols[:, t : t + 1], (IMPS, OWNERS))
        row = jnp.broadcast_to(row_cols[:, t : t + 1], (IMPS, OWNERS))
        for r in range(CAP):
            target = iota((IMPS, OWNERS), 1) * LINES + (CAP * t + r)
            lines.append(jnp.sum(jnp.where(slot == target, row, 0), axis=0, keepdims=True))
    want_ref[...] = jnp.transpose(jnp.concatenate(lines, axis=0))


def serve_kernel(req_ref, tab_ref, out_ref, wide_ref):
    req = req_ref[...]
    half = ROWS // 2
    for t in range(TABLES):
        table = jnp.concatenate([tab_ref[t, :half, :], tab_ref[t, half:, :]], axis=1)
        for r in range(CAP):
            j = CAP * t + r
            row = req[:, j : j + 1]
            hot = hot_rows(row & 127, (row >> 7) & 15, 16)
            both = jnp.dot(hot, table, preferred_element_type=F32)
            upper = jnp.broadcast_to(row, (OWNERS, EMB)) >= half
            wide_ref[pl.ds(j, OWNERS, stride=LINES), :] = jnp.where(
                upper, both[:, EMB:], both[:, :EMB]
            )
    out_ref[...] = wide_ref[...].astype(BF).reshape(OWNERS, LINES, EMB)


def step_kernel(
    ret_ref, slot_ref, slot_col_ref, ses_ref, rel_ref, lb_ref, w_ref, b_ref, ws_ref,
    out_ref, dense_ref,
):
    back = ret_ref[...].reshape(OWNERS * LINES, EMB)
    half = OWNERS * LINES // 2
    source = jnp.concatenate([back[:half], back[half:]], axis=1)
    slot_cols = slot_col_ref[...]
    pieces = []
    for t in range(TABLES):
        slot = slot_cols[:, t : t + 1]
        both = jnp.dot(hot_rows(slot & 127, (slot >> 7) & 7, 8), source, preferred_element_type=F32)
        upper = jnp.broadcast_to(slot, (IMPS, EMB)) >= half
        pieces.append(jnp.where(upper, both[:, EMB:], both[:, :EMB]).astype(BF))
    inputs = jnp.concatenate(pieces, axis=1)
    w_bf = w_ref[...].astype(BF)
    w_score = ws_ref[...]
    pre = jnp.dot(inputs, w_bf, preferred_element_type=F32) + b_ref[...]
    sig = jax.nn.sigmoid(pre)
    hidden = pre * sig
    aux = jnp.transpose(
        jnp.concatenate(
            [rel_ref[...], lb_ref[...], ses_ref[...].astype(F32)] + [rel_ref[...]] * 5, axis=0
        )
    )
    relevance, bias_col, session = aux[:, 0:1], aux[:, 1:2], aux[:, 2:3]
    scores = jnp.sum(hidden * w_score, axis=1, keepdims=True) + bias_col
    first = session < 0.5
    low = jnp.float32(-jnp.inf)
    top = [jnp.max(jnp.where(m, scores, low), axis=0, keepdims=True) for m in (first, ~first)]
    shifted = scores - jnp.where(first, top[0], top[1])
    exponent = jnp.exp(shifted)
    total = [jnp.sum(jnp.where(m, exponent, 0.0), axis=0, keepdims=True) for m in (first, ~first)]
    weight = [jnp.sum(jnp.where(m, relevance, 0.0), axis=0, keepdims=True) for m in (first, ~first)]
    probability = exponent / jnp.where(first, total[0], total[1])
    target = relevance / jnp.where(first, weight[0], weight[1])
    loss = jnp.log(total[0]) + jnp.log(total[1]) - jnp.sum(target * shifted, axis=0, keepdims=True)
    score_grad = probability - target
    pre_grad = score_grad * w_score * (sig * (1.0 + pre * (1.0 - sig)))
    pre_grad_bf = pre_grad.astype(BF)
    grad = jnp.dot(pre_grad_bf, w_bf.T, preferred_element_type=F32).astype(BF)
    slots = slot_ref[...]
    values, hots = [], []
    for t in range(TABLES):
        piece = grad[:, t * EMB : (t + 1) * EMB]
        upper = jnp.broadcast_to(slot_cols[:, t : t + 1], (IMPS, EMB)) >= half
        zero = jnp.zeros((IMPS, EMB), BF)
        values.append(
            jnp.concatenate([jnp.where(upper, zero, piece), jnp.where(upper, piece, zero)], axis=1)
        )
        slot = slots[t : t + 1]
        hots.append(hot_cols(slot & 127, (slot >> 7) & 7, 8))
    placed = jnp.dot(
        jnp.concatenate(hots, axis=1), jnp.concatenate(values, axis=0), preferred_element_type=F32
    )
    out_ref[: OWNERS // 2] = placed[:, :EMB].astype(BF).reshape(OWNERS // 2, LINES, EMB)
    out_ref[OWNERS // 2 :] = placed[:, EMB:].astype(BF).reshape(OWNERS // 2, LINES, EMB)
    weight_grad = lax.dot_general(
        inputs, pre_grad_bf, (((0,), (0,)), ((), ())), preferred_element_type=F32
    )
    dense_ref[:, 0:HID] = weight_grad[:256]
    dense_ref[:, HID : 2 * HID] = weight_grad[256:]
    bias_grad = jnp.sum(pre_grad, axis=0, keepdims=True)
    score_w_grad = jnp.sum(score_grad * hidden, axis=0, keepdims=True)
    dense_ref[:, 2 * HID :] = jnp.zeros((256, 128), F32)
    for k in range(4):
        dense_ref[k : k + 1, 2 * HID :] = bias_grad[:, 128 * k : 128 * (k + 1)]
        dense_ref[4 + k : 5 + k, 2 * HID :] = score_w_grad[:, 128 * k : 128 * (k + 1)]
    dense_ref[8:9, 2 * HID :] = jnp.broadcast_to(loss, (1, 128))


def place_kernel(core_ref, own_ref, other_ref, own_id_ref, other_id_ref, out_ref, wide_ref, buf_ref, sems):
    core = core_ref[0]
    lines = OWNERS * LINES
    wide_ref[:lines] = own_ref[...].reshape(lines, EMB).astype(F32)
    wide_ref[lines:] = other_ref[...].reshape(lines, EMB).astype(F32)
    cols = [own_id_ref[...], other_id_ref[...]]
    rows = [jnp.transpose(c) for c in cols]
    copies = []
    for t in range(TABLES):
        values, hots = [], []
        for s in range(2):
            for r in range(CAP):
                j = CAP * t + r
                line = wide_ref[pl.ds(s * lines + j, OWNERS, stride=LINES), :]
                quarter = jnp.broadcast_to(cols[s][:, j : j + 1] >> 10, (OWNERS, EMB)) - 2 * core
                values.append(
                    jnp.concatenate(
                        [jnp.where(quarter == 0, line, 0.0), jnp.where(quarter == 1, line, 0.0)],
                        axis=1,
                    ).astype(BF)
                )
                row = rows[s][j : j + 1]
                hots.append(hot_cols(row & 127, (row >> 7) & 7, 8))
        total = jnp.dot(
            jnp.concatenate(hots, axis=1), jnp.concatenate(values, axis=0), preferred_element_type=F32
        )
        for h in range(2):
            x = total[:, h * EMB : (h + 1) * EMB]
            mean = jnp.sum(x * x, axis=1, keepdims=True) * (1.0 / EMB)
            buf_ref[t, 1024 * h : 1024 * (h + 1)] = x * (1.0 / (jnp.sqrt(mean) + 1e-06))
        copy = pltpu.make_async_copy(buf_ref.at[t], out_ref.at[t], sems.at[t])
        copy.start()
        copies.append(copy)
    for copy in copies:
        copy.wait()


def final_kernel(dense_ref, w_ref, b_ref, s_ref, loss_ref):
    main = dense_ref[:, : 2 * HID]
    small = dense_ref[0:8, 2 * HID :]
    square = jnp.sum(jnp.sum(main * main, axis=0, keepdims=True), axis=1, keepdims=True) + jnp.sum(
        jnp.sum(small * small, axis=0, keepdims=True), axis=1, keepdims=True
    )
    factor = 1.0 / jnp.sqrt(square * (1.0 / (HID * HID + 2 * HID)) + 1e-06)
    w_ref[:256] = main[:, :HID] * factor
    w_ref[256:] = main[:, HID:] * factor
    b_ref[...] = small[0:4] * factor
    s_ref[...] = small[4:8] * factor
    loss_ref[...] = dense_ref[8:9, 2 * HID :] * (1.0 / 512)


def sds(shape, dtype):
    return jax.ShapeDtypeStruct(shape, dtype)


def cost(flops, moved):
    return pl.CostEstimate(flops=flops, bytes_accessed=moved, transcendentals=0)


def around(axis, step):
    n = lax.axis_size(axis)
    return [(i, (i + step) % n) for i in range(n)]


def scattered_sum(whole, axis):
    n = lax.axis_size(axis)
    me = lax.axis_index(axis)
    size = whole.shape[0] // n
    total = lax.dynamic_slice_in_dim(whole, me * size, size, 0)
    arrived = [
        lax.ppermute(
            lax.dynamic_slice_in_dim(whole, ((me + d) % n) * size, size, 0), axis, around(axis, d)
        )
        for d in range(1, n)
    ]
    for a in arrived:
        total = total + a
    return total


def gathered(part, axis):
    n = lax.axis_size(axis)
    me = lax.axis_index(axis)
    size = part.shape[0]
    whole = jnp.zeros((n * size, part.shape[1]), part.dtype)
    whole = lax.dynamic_update_slice_in_dim(whole, part, me * size, 0)
    for d in range(1, n):
        arrived = lax.ppermute(part, axis, around(axis, d))
        whole = lax.dynamic_update_slice_in_dim(whole, arrived, ((me - d) % n) * size, 0)
    return whole


def on_device(
    tables, owner_ids, row_ids, session_of, relevance, logit_bias, w_hidden, bias_hidden, w_score
):
    wanted, slots, slot_cols = pl.pallas_call(
        slots_kernel,
        out_shape=(
            sds((OWNERS, LINES), jnp.int32),
            sds((TABLES, IMPS), jnp.int32),
            sds((IMPS, 2 * TABLES), jnp.int32),
        ),
        in_specs=[VMEM, VMEM],
        out_specs=(VMEM, VMEM, VMEM),
        cost_estimate=cost(1 << 20, 1 << 16),
        name="slots",
    )(owner_ids.reshape(8, 128), row_ids.reshape(TABLES, IMPS))
    requested = lax.all_to_all(wanted, TABLE, split_axis=0, concat_axis=0, tiled=True)
    other_ids = lax.ppermute(requested, "dp", [(0, 1), (1, 0)])
    served = pl.pallas_call(
        serve_kernel,
        out_shape=sds((OWNERS, LINES, EMB), BF),
        in_specs=[VMEM, VMEM],
        out_specs=VMEM,
        scratch_shapes=[pltpu.VMEM((OWNERS * LINES, EMB), F32)],
        cost_estimate=cost(4 << 30, 5 << 20),
        name="serve",
    )(requested, tables)
    returned = lax.all_to_all(served, TABLE, split_axis=0, concat_axis=0, tiled=True)
    outgoing, dense = pl.pallas_call(
        step_kernel,
        out_shape=(sds((OWNERS, LINES, EMB), BF), sds((256, 2 * HID + 128), F32)),
        in_specs=[VMEM] * 9,
        out_specs=(VMEM, VMEM),
        cost_estimate=cost(3 << 30, 3 << 20),
        name="step",
    )(
        returned, slots, slot_cols, session_of, relevance, logit_bias, w_hidden,
        bias_hidden.reshape(1, HID), w_score.reshape(1, HID),
    )
    incoming = lax.all_to_all(outgoing, TABLE, split_axis=0, concat_axis=0, tiled=True)
    other = lax.ppermute(incoming, "dp", [(0, 1), (1, 0)])
    core = lax.axis_index("dp").astype(jnp.int32).reshape(1)
    emb_step = pl.pallas_call(
        place_kernel,
        out_shape=sds((TABLES, ROWS // 2, EMB), F32),
        in_specs=[pl.BlockSpec(memory_space=pltpu.SMEM)] + [VMEM] * 4,
        out_specs=ANY,
        scratch_shapes=[
            pltpu.VMEM((2 * OWNERS * LINES, EMB), F32),
            pltpu.VMEM((TABLES, ROWS // 2, EMB), F32),
            pltpu.SemaphoreType.DMA((TABLES,)),
        ],
        cost_estimate=cost(4 << 30, 5 << 20),
        name="place",
    )(core, incoming, other, requested, other_ids)
    total = dense
    for axis in ("dp", "y", "x", "z"):
        total = scattered_sum(total, axis)
    for axis in ("z", "x", "y", "dp"):
        total = gathered(total, axis)
    step_hidden, step_bias, step_score, loss = pl.pallas_call(
        final_kernel,
        out_shape=(
            sds((HID, HID), F32), sds((4, 128), F32), sds((4, 128), F32), sds((1, 128), F32),
        ),
        in_specs=[VMEM],
        out_specs=(VMEM,) * 4,
        cost_estimate=cost(1 << 20, 2 << 20),
        name="final",
    )(total)
    return emb_step, step_hidden, step_bias.reshape(HID), step_score.reshape(HID), loss[0, 0]


def solution(mesh):
    split = Mesh(mesh.devices.reshape(4, 8, 4, mesh.shape["dp"]), ALL)
    return jax.shard_map(
        on_device,
        mesh=split,
        in_specs=(
            P(None, TABLE, None),
            P(ALL, None, None, None),
            P(ALL, None, None),
            P(ALL, None),
            P(ALL, None),
            P(ALL, None),
            P(),
            P(),
            P(),
        ),
        out_specs=(P(None, ALL, None), P(), P(), P(), P()),
        check_vma=False,
    )
```

```python
import jax
import jax.numpy as jnp
from jax import lax
from jax.experimental import pallas as pl
from jax.experimental.pallas import tpu as pltpu
from jax.sharding import Mesh
from jax.sharding import PartitionSpec as P


TABLE = ("x", "z", "y")
ALL = ("x", "z", "y", "dp")
TABLES = 4
CAP = 4
LINES = TABLES * CAP
OWNERS = 128
IMPS = 256
EMB = 128
ROWS = 4096
HID = 512
DENSE = 2 * HID + 128
VMEM = pl.BlockSpec(memory_space=pltpu.VMEM)
ANY = pl.BlockSpec(memory_space=pl.ANY)
BF = jnp.bfloat16
F32 = jnp.float32


def iota(shape, dim):
    return lax.broadcasted_iota(jnp.int32, shape, dim)


def hot_rows(low, block, blocks):
    n = low.shape[0]
    one = jnp.where(iota((n, 128), 1) == low, 1.0, 0.0).astype(BF)
    which = jnp.broadcast_to(block, (n, 128)).astype(F32).astype(BF)
    zero = jnp.zeros((n, 128), BF)
    return jnp.concatenate([jnp.where(which == BF(c), one, zero) for c in range(blocks)], axis=1)


def hot_cols(low, block, blocks):
    n = low.shape[1]
    one = jnp.where(iota((128, n), 0) == low, 1.0, 0.0).astype(BF)
    which = jnp.broadcast_to(block, (128, n)).astype(F32).astype(BF)
    zero = jnp.zeros((128, n), BF)
    return jnp.concatenate([jnp.where(which == BF(c), one, zero) for c in range(blocks)], axis=0)


def slots_kernel(own_ref, row_ref, want_ref, slot_ref, slot_col_ref):
    own = own_ref[...]
    own_rows = [
        jnp.concatenate([own[2 * t : 2 * t + 1], own[2 * t + 1 : 2 * t + 2]], axis=1)
        for t in range(TABLES)
    ]
    own_cols = jnp.transpose(jnp.concatenate(own_rows + own_rows, axis=0))
    row_cols = jnp.transpose(jnp.concatenate([row_ref[...], row_ref[...]], axis=0))
    before = iota((IMPS, IMPS), 0) < iota((IMPS, IMPS), 1)
    slots = []
    for t in range(TABLES):
        same = (own_cols[:, t : t + 1] == own_rows[t]) & before
        rank = jnp.sum(jnp.where(same, 1, 0), axis=0, keepdims=True)
        slots.append(own_rows[t] * LINES + (CAP * t) + rank)
    slot_ref[...] = jnp.concatenate(slots, axis=0)
    slot_cols = jnp.transpose(jnp.concatenate(slots + slots, axis=0))
    slot_col_ref[...] = slot_cols
    lines = []
    for t in range(TABLES):
        slot = jnp.broadcast_to(slot_cols[:, t : t + 1], (IMPS, OWNERS))
        row = jnp.broadcast_to(row_cols[:, t : t + 1], (IMPS, OWNERS))
        for r in range(CAP):
            target = iota((IMPS, OWNERS), 1) * LINES + (CAP * t + r)
            lines.append(jnp.sum(jnp.where(slot == target, row, 0), axis=0, keepdims=True))
    want_ref[...] = jnp.transpose(jnp.concatenate(lines, axis=0))


def serve_kernel(req_ref, far_ref, out_ref, wide_ref, tab_ref, sems):
    copies = [pltpu.make_async_copy(far_ref.at[t], tab_ref.at[t], sems.at[t]) for t in range(TABLES)]
    for copy in copies:
        copy.start()
    req = req_ref[...]
    half = ROWS // 2
    for t in range(TABLES):
        copies[t].wait()
        table = jnp.concatenate([tab_ref[t, :half, :], tab_ref[t, half:, :]], axis=1)
        rows = [req[:, CAP * t + r : CAP * t + r + 1] for r in range(CAP)]
        hot = jnp.concatenate([hot_rows(row & 127, (row >> 7) & 15, 16) for row in rows], axis=0)
        both = jnp.dot(hot, table, preferred_element_type=F32)
        for r in range(CAP):
            upper = jnp.broadcast_to(rows[r], (OWNERS, EMB)) >= half
            mine = both[r * OWNERS : (r + 1) * OWNERS]
            wide_ref[pl.ds(CAP * t + r, OWNERS, stride=LINES), :] = jnp.where(
                upper, mine[:, EMB:], mine[:, :EMB]
            )
    out_ref[...] = wide_ref[...].astype(BF).reshape(OWNERS, LINES, EMB)


def step_kernel(
    core_ref, ret_ref, slot_ref, slot_col_ref, ses_ref, rel_ref, lb_ref, w_ref, b_ref, ws_ref,
    out_ref, keep_ref, send_ref, dense_ref,
):
    back = ret_ref[...].reshape(OWNERS * LINES, EMB)
    half = OWNERS * LINES // 2
    source = jnp.concatenate([back[:half], back[half:]], axis=1)
    slot_cols = slot_col_ref[...]
    pieces = []
    picks = []
    for t in range(TABLES):
        slot = slot_cols[:, t : t + 1]
        picks.append(hot_rows(slot & 127, (slot >> 7) & 7, 8))
    found = jnp.dot(jnp.concatenate(picks, axis=0), source, preferred_element_type=F32)
    for t in range(TABLES):
        both = found[t * IMPS : (t + 1) * IMPS]
        upper = jnp.broadcast_to(slot_cols[:, t : t + 1], (IMPS, EMB)) >= half
        pieces.append(jnp.where(upper, both[:, EMB:], both[:, :EMB]).astype(BF))
    inputs = jnp.concatenate(pieces, axis=1)
    w_bf = w_ref[...].astype(BF)
    w_score = ws_ref[...]
    pre = jnp.dot(inputs, w_bf, preferred_element_type=F32) + b_ref[...]
    sig = jax.nn.sigmoid(pre)
    hidden = pre * sig
    aux = jnp.transpose(
        jnp.concatenate(
            [rel_ref[...], lb_ref[...], ses_ref[...].astype(F32)] + [rel_ref[...]] * 5, axis=0
        )
    )
    relevance, bias_col, session = aux[:, 0:1], aux[:, 1:2], aux[:, 2:3]
    scores = jnp.sum(hidden * w_score, axis=1, keepdims=True) + bias_col
    first = session < 0.5
    low = jnp.float32(-jnp.inf)
    top = [jnp.max(jnp.where(m, scores, low), axis=0, keepdims=True) for m in (first, ~first)]
    shifted = scores - jnp.where(first, top[0], top[1])
    exponent = jnp.exp(shifted)
    total = [jnp.sum(jnp.where(m, exponent, 0.0), axis=0, keepdims=True) for m in (first, ~first)]
    weight = [jnp.sum(jnp.where(m, relevance, 0.0), axis=0, keepdims=True) for m in (first, ~first)]
    probability = exponent / jnp.where(first, total[0], total[1])
    target = relevance / jnp.where(first, weight[0], weight[1])
    loss = jnp.log(total[0]) + jnp.log(total[1]) - jnp.sum(target * shifted, axis=0, keepdims=True)
    score_grad = probability - target
    pre_grad = score_grad * w_score * (sig * (1.0 + pre * (1.0 - sig)))
    pre_grad_bf = pre_grad.astype(BF)
    grad = jnp.dot(pre_grad_bf, w_bf.T, preferred_element_type=F32).astype(BF)
    slots = slot_ref[...]
    values, hots = [], []
    for t in range(TABLES):
        slot = slots[t : t + 1]
        hots.append(hot_cols(slot & 127, (slot >> 7) & 7, 8))
        piece = grad[:, t * EMB : (t + 1) * EMB]
        upper = jnp.broadcast_to(slot_cols[:, t : t + 1], (IMPS, EMB)) >= half
        zero = jnp.zeros((IMPS, EMB), BF)
        values.append(
            jnp.concatenate([jnp.where(upper, zero, piece), jnp.where(upper, piece, zero)], axis=1)
        )
    placed = jnp.dot(
        jnp.concatenate(hots, axis=1), jnp.concatenate(values, axis=0), preferred_element_type=F32
    )
    out_ref[: OWNERS // 2] = placed[:, :EMB].astype(BF).reshape(OWNERS // 2, LINES, EMB)
    out_ref[OWNERS // 2 :] = placed[:, EMB:].astype(BF).reshape(OWNERS // 2, LINES, EMB)
    weight_grad = lax.dot_general(
        inputs, pre_grad_bf, (((0,), (0,)), ((), ())), preferred_element_type=F32
    )
    dense_ref[:, 0:HID] = weight_grad[:256]
    dense_ref[:, HID : 2 * HID] = weight_grad[256:]
    bias_grad = jnp.sum(pre_grad, axis=0, keepdims=True)
    score_w_grad = jnp.sum(score_grad * hidden, axis=0, keepdims=True)
    dense_ref[:, 2 * HID :] = jnp.zeros((256, 128), F32)
    for k in range(4):
        dense_ref[k : k + 1, 2 * HID :] = bias_grad[:, 128 * k : 128 * (k + 1)]
        dense_ref[4 + k : 5 + k, 2 * HID :] = score_w_grad[:, 128 * k : 128 * (k + 1)]
    dense_ref[8:9, 2 * HID :] = jnp.broadcast_to(loss, (1, 128))
    start = pl.multiple_of(core_ref[0] * 128, 128)
    keep_ref[...] = dense_ref[pl.ds(start, 128), :]
    send_ref[...] = dense_ref[pl.ds(128 - start, 128), :]


def place_kernel(
    core_ref, own_ref, other_ref, own_id_ref, other_id_ref, out_ref, wide_ref, buf_ref, sems
):
    core = core_ref[0]
    lines = OWNERS * LINES
    wide_ref[:lines] = own_ref[...].reshape(lines, EMB).astype(F32)
    wide_ref[lines:] = other_ref[...].reshape(lines, EMB).astype(F32)
    cols = [own_id_ref[...], other_id_ref[...]]
    rows = [jnp.transpose(c) for c in cols]
    copies = []
    for t in range(TABLES):
        values, hots = [], []
        for s in range(2):
            for r in range(CAP):
                j = CAP * t + r
                line = wide_ref[pl.ds(s * lines + j, OWNERS, stride=LINES), :]
                quarter = jnp.broadcast_to(cols[s][:, j : j + 1] >> 10, (OWNERS, EMB)) - 2 * core
                values.append(
                    jnp.concatenate(
                        [jnp.where(quarter == 0, line, 0.0), jnp.where(quarter == 1, line, 0.0)],
                        axis=1,
                    ).astype(BF)
                )
                row = rows[s][j : j + 1]
                hots.append(hot_cols(row & 127, (row >> 7) & 7, 8))
        total = jnp.dot(
            jnp.concatenate(hots, axis=1), jnp.concatenate(values, axis=0), preferred_element_type=F32
        )
        for h in range(2):
            x = total[:, h * EMB : (h + 1) * EMB]
            mean = jnp.sum(x * x, axis=1, keepdims=True) * (1.0 / EMB)
            buf_ref[t, 1024 * h : 1024 * (h + 1)] = x * (1.0 / (jnp.sqrt(mean) + 1e-06))
        copy = pltpu.make_async_copy(buf_ref.at[t], out_ref.at[t], sems.at[t])
        copy.start()
        copies.append(copy)
    for copy in copies:
        copy.wait()


def final_kernel(core_ref, own_ref, other_ref, w_ref, b_ref, s_ref, loss_ref, dense_ref):
    start = pl.multiple_of(core_ref[0] * 128, 128)
    dense_ref[pl.ds(start, 128), :] = own_ref[...]
    dense_ref[pl.ds(128 - start, 128), :] = other_ref[...]
    main = dense_ref[:, : 2 * HID]
    small = dense_ref[0:8, 2 * HID :]
    square = jnp.sum(jnp.sum(main * main, axis=0, keepdims=True), axis=1, keepdims=True) + jnp.sum(
        jnp.sum(small * small, axis=0, keepdims=True), axis=1, keepdims=True
    )
    factor = 1.0 / jnp.sqrt(square * (1.0 / (HID * HID + 2 * HID)) + 1e-06)
    w_ref[:256] = main[:, :HID] * factor
    w_ref[256:] = main[:, HID:] * factor
    b_ref[...] = small[0:4] * factor
    s_ref[...] = small[4:8] * factor
    loss_ref[...] = dense_ref[8:9, 2 * HID :] * (1.0 / 512)


def sds(shape, dtype):
    return jax.ShapeDtypeStruct(shape, dtype)


def cost(flops, moved):
    return pl.CostEstimate(flops=flops, bytes_accessed=moved, transcendentals=0)


def whole_step(
    tables, owner_ids, row_ids, session_of, relevance, logit_bias, w_hidden, bias_hidden, w_score
):
    core = lax.axis_index("dp").astype(jnp.int32).reshape(1)
    swap = [(0, 1), (1, 0)]
    smem = pl.BlockSpec(memory_space=pltpu.SMEM)
    wanted, slots, slot_cols = pl.pallas_call(
        slots_kernel,
        out_shape=(
            sds((OWNERS, LINES), jnp.int32),
            sds((TABLES, IMPS), jnp.int32),
            sds((IMPS, 2 * TABLES), jnp.int32),
        ),
        in_specs=[VMEM, VMEM],
        out_specs=(VMEM, VMEM, VMEM),
        cost_estimate=cost(1 << 20, 1 << 16),
        compiler_params=pltpu.CompilerParams(vmem_limit_bytes=8 << 20),
        name="slots",
    )(owner_ids.reshape(8, 128), row_ids.reshape(TABLES, IMPS))
    requested = lax.all_to_all(wanted, TABLE, split_axis=0, concat_axis=0, tiled=True)
    other_ids = lax.ppermute(requested, "dp", swap)
    served = pl.pallas_call(
        serve_kernel,
        out_shape=sds((OWNERS, LINES, EMB), BF),
        in_specs=[VMEM, pl.BlockSpec(memory_space=pltpu.HBM)],
        out_specs=VMEM,
        scratch_shapes=[
            pltpu.VMEM((OWNERS * LINES, EMB), F32),
            pltpu.VMEM((TABLES, ROWS, EMB), BF),
            pltpu.SemaphoreType.DMA((TABLES,)),
        ],
        cost_estimate=cost(4 << 30, 5 << 20),
        compiler_params=pltpu.CompilerParams(vmem_limit_bytes=61 << 20),
        name="serve",
    )(requested, tables)
    returned = lax.all_to_all(served, TABLE, split_axis=0, concat_axis=0, tiled=True)
    outgoing, keep, send = pl.pallas_call(
        step_kernel,
        out_shape=(
            sds((OWNERS, LINES, EMB), BF), sds((128, DENSE), F32), sds((128, DENSE), F32),
        ),
        in_specs=[smem] + [VMEM] * 9,
        out_specs=(VMEM,) * 3,
        scratch_shapes=[pltpu.VMEM((256, DENSE), F32)],
        cost_estimate=cost(3 << 30, 3 << 20),
        compiler_params=pltpu.CompilerParams(vmem_limit_bytes=24 << 20),
        name="step",
    )(
        core, returned, slots, slot_cols, session_of, relevance, logit_bias, w_hidden,
        bias_hidden.reshape(1, HID), w_score.reshape(1, HID),
    )
    incoming = lax.all_to_all(outgoing, TABLE, split_axis=0, concat_axis=0, tiled=True)
    chip = keep + lax.ppermute(send, "dp", swap)
    plane = lax.all_to_all(
        chip.reshape(16, 8, DENSE), ("x", "y"), split_axis=0, concat_axis=0, tiled=True
    ).sum(axis=0)
    total = lax.all_to_all(
        jnp.broadcast_to(plane[None], (8, 8, DENSE)), "z", split_axis=0, concat_axis=0, tiled=True
    ).sum(axis=0)
    mine = lax.all_to_all(
        jnp.broadcast_to(total[None], (16, 8, DENSE)), ("x", "y"),
        split_axis=0, concat_axis=0, tiled=True,
    ).reshape(128, DENSE)
    theirs = lax.ppermute(mine, "dp", swap)
    other = lax.ppermute(incoming, "dp", swap)
    emb_step = pl.pallas_call(
        place_kernel,
        out_shape=sds((TABLES, ROWS // 2, EMB), F32),
        in_specs=[smem] + [VMEM] * 4,
        out_specs=ANY,
        scratch_shapes=[
            pltpu.VMEM((2 * OWNERS * LINES, EMB), F32),
            pltpu.VMEM((TABLES, ROWS // 2, EMB), F32),
            pltpu.SemaphoreType.DMA((TABLES,)),
        ],
        cost_estimate=cost(4 << 30, 5 << 20),
        compiler_params=pltpu.CompilerParams(vmem_limit_bytes=28 << 20),
        name="place",
    )(core, incoming, other, requested, other_ids)
    step_hidden, step_bias, step_score, loss = pl.pallas_call(
        final_kernel,
        out_shape=(
            sds((HID, HID), F32), sds((4, 128), F32), sds((4, 128), F32), sds((1, 128), F32),
        ),
        in_specs=[smem, VMEM, VMEM],
        out_specs=(VMEM,) * 4,
        scratch_shapes=[pltpu.VMEM((256, DENSE), F32)],
        cost_estimate=cost(1 << 20, 2 << 20),
        compiler_params=pltpu.CompilerParams(vmem_limit_bytes=12 << 20),
        name="final",
    )(core, mine, theirs)
    return emb_step, step_hidden, step_bias.reshape(HID), step_score.reshape(HID), loss[0, 0]


def solution(mesh):
    split = Mesh(mesh.devices.reshape(4, 8, 4, mesh.shape["dp"]), ALL)
    return jax.shard_map(
        whole_step,
        mesh=split,
        in_specs=(
            P(None, TABLE, None),
            P(ALL, None, None, None),
            P(ALL, None, None),
            P(ALL, None),
            P(ALL, None),
            P(ALL, None),
            P(),
            P(),
            P(),
        ),
        out_specs=(P(None, ALL, None), P(), P(), P(), P()),
        check_vma=False,
    )
```

```python
import jax
import jax.numpy as jnp
from jax import lax
from jax.experimental import pallas as pl
from jax.experimental.pallas import tpu as pltpu
from jax.sharding import Mesh
from jax.sharding import PartitionSpec as P


TABLE = ("x", "z", "y")
ALL = ("x", "z", "y", "dp")
TABLES = 4
CAP = 4
LINES = TABLES * CAP
OWNERS = 128
IMPS = 256
EMB = 128
ROWS = 4096
HID = 512
FOLD = 4
SMALL = 16
VMEM = pl.BlockSpec(memory_space=pltpu.VMEM)
ANY = pl.BlockSpec(memory_space=pl.ANY)
BF = jnp.bfloat16
F32 = jnp.float32


HBM = pl.BlockSpec(memory_space=pltpu.HBM)
SMEM = pl.BlockSpec(memory_space=pltpu.SMEM)


def iota(shape, dim):
    return lax.broadcasted_iota(jnp.int32, shape, dim)


def hot_rows(low, block, blocks):
    n = low.shape[0]
    one = jnp.where(iota((n, 128), 1) == low, 1.0, 0.0).astype(BF)
    which = jnp.broadcast_to(block, (n, 128)).astype(F32).astype(BF)
    zero = jnp.zeros((n, 128), BF)
    return jnp.concatenate([jnp.where(which == BF(c), one, zero) for c in range(blocks)], axis=1)


def hot_cols(low, block, blocks):
    n = low.shape[1]
    one = jnp.where(iota((128, n), 0) == low, 1.0, 0.0).astype(BF)
    which = jnp.broadcast_to(block, (128, n)).astype(F32).astype(BF)
    zero = jnp.zeros((128, n), BF)
    return jnp.concatenate([jnp.where(which == BF(c), one, zero) for c in range(blocks)], axis=0)


def chosen(wide, which):
    kept = wide[:, :EMB]
    for f in range(1, FOLD):
        kept = jnp.where(which == f, wide[:, f * EMB : (f + 1) * EMB], kept)
    return kept


def fanned(piece, which):
    zero = jnp.zeros_like(piece)
    return jnp.concatenate([jnp.where(which == f, piece, zero) for f in range(FOLD)], axis=1)


def slots_kernel(own_hbm, row_hbm, want_ref, slot_ref, slot_col_ref, own_ref, row_ref, sems):
    copies = [
        pltpu.make_async_copy(own_hbm, own_ref, sems.at[0]),
        pltpu.make_async_copy(row_hbm, row_ref, sems.at[1]),
    ]
    for copy in copies:
        copy.start()
    for copy in copies:
        copy.wait()
    own = own_ref[...]
    own_rows = [
        jnp.concatenate([own[2 * t : 2 * t + 1], own[2 * t + 1 : 2 * t + 2]], axis=1)
        for t in range(TABLES)
    ]
    own_cols = jnp.transpose(jnp.concatenate(own_rows + own_rows, axis=0))
    row_cols = jnp.transpose(jnp.concatenate([row_ref[...], row_ref[...]], axis=0))
    before = iota((IMPS, IMPS), 0) < iota((IMPS, IMPS), 1)
    slots = []
    for t in range(TABLES):
        same = (own_cols[:, t : t + 1] == own_rows[t]) & before
        rank = jnp.sum(jnp.where(same, 1, 0), axis=0, keepdims=True)
        slots.append(own_rows[t] * LINES + (CAP * t) + rank)
    slot_ref[...] = jnp.concatenate(slots, axis=0)
    slot_cols = jnp.transpose(jnp.concatenate(slots + slots, axis=0))
    slot_col_ref[...] = slot_cols
    lines = []
    for t in range(TABLES):
        slot = jnp.broadcast_to(slot_cols[:, t : t + 1], (IMPS, OWNERS))
        row = jnp.broadcast_to(row_cols[:, t : t + 1], (IMPS, OWNERS))
        for r in range(CAP):
            target = iota((IMPS, OWNERS), 1) * LINES + (CAP * t + r)
            lines.append(jnp.sum(jnp.where(slot == target, row, 0), axis=0, keepdims=True))
    want_ref[...] = jnp.transpose(jnp.concatenate(lines, axis=0))


def serve_kernel(req_ref, far_ref, out_ref, wide_ref, tab_ref, sems):
    copies = [pltpu.make_async_copy(far_ref.at[t], tab_ref.at[t], sems.at[t]) for t in range(TABLES)]
    for copy in copies:
        copy.start()
    req = req_ref[...]
    part = ROWS // FOLD
    for t in range(TABLES):
        rows = [req[:, CAP * t + r : CAP * t + r + 1] for r in range(CAP)]
        hot = jnp.concatenate([hot_rows(row & 127, (row >> 7) & 7, 8) for row in rows], axis=0)
        copies[t].wait()
        table = jnp.concatenate(
            [tab_ref[t, f * part : (f + 1) * part, :] for f in range(FOLD)], axis=1
        )
        wide = jnp.dot(hot, table, preferred_element_type=F32)
        for r in range(CAP):
            which = jnp.broadcast_to(rows[r] >> 10, (OWNERS, EMB))
            wide_ref[pl.ds(CAP * t + r, OWNERS, stride=LINES), :] = chosen(
                wide[r * OWNERS : (r + 1) * OWNERS], which
            )
    out_ref[...] = wide_ref[...].astype(BF).reshape(OWNERS, LINES, EMB)


def step_kernel(
    core_ref, ret_ref, slot_col_ref, ses_ref, rel_ref, lb_ref, w_ref, b_ref, ws_ref,
    pre_grad_ref, keep_ref, send_ref, dense_ref,
):
    back = ret_ref[...].reshape(OWNERS * LINES, EMB)
    half = OWNERS * LINES // 2
    source = jnp.concatenate([back[:half], back[half:]], axis=1)
    slot_cols = slot_col_ref[...]
    pieces = []
    for t in range(TABLES):
        slot = slot_cols[:, t : t + 1]
        both = jnp.dot(hot_rows(slot & 127, (slot >> 7) & 7, 8), source, preferred_element_type=F32)
        upper = jnp.broadcast_to(slot, (IMPS, EMB)) >= half
        pieces.append(jnp.where(upper, both[:, EMB:], both[:, :EMB]).astype(BF))
    inputs = jnp.concatenate(pieces, axis=1)
    w_bf = w_ref[...].astype(BF)
    w_score = ws_ref[...]
    pre = jnp.dot(inputs, w_bf, preferred_element_type=F32) + b_ref[...]
    sig = jax.nn.sigmoid(pre)
    hidden = pre * sig
    aux = jnp.transpose(
        jnp.concatenate(
            [rel_ref[...], lb_ref[...], ses_ref[...].astype(F32)] + [rel_ref[...]] * 5, axis=0
        )
    )
    relevance, bias_col, session = aux[:, 0:1], aux[:, 1:2], aux[:, 2:3]
    scores = jnp.sum(hidden * w_score, axis=1, keepdims=True) + bias_col
    first = session < 0.5
    low = jnp.float32(-jnp.inf)
    top = [jnp.max(jnp.where(m, scores, low), axis=0, keepdims=True) for m in (first, ~first)]
    shifted = scores - jnp.where(first, top[0], top[1])
    exponent = jnp.exp(shifted)
    total = [jnp.sum(jnp.where(m, exponent, 0.0), axis=0, keepdims=True) for m in (first, ~first)]
    weight = [jnp.sum(jnp.where(m, relevance, 0.0), axis=0, keepdims=True) for m in (first, ~first)]
    probability = exponent / jnp.where(first, total[0], total[1])
    target = relevance / jnp.where(first, weight[0], weight[1])
    loss = jnp.log(total[0]) + jnp.log(total[1]) - jnp.sum(target * shifted, axis=0, keepdims=True)
    score_grad = probability - target
    pre_grad = score_grad * w_score * (sig * (1.0 + pre * (1.0 - sig)))
    pre_grad_bf = pre_grad.astype(BF)
    pre_grad_ref[...] = pre_grad_bf
    dense_ref[...] = lax.dot_general(
        inputs, pre_grad_bf, (((0,), (0,)), ((), ())), preferred_element_type=F32
    )
    bias_grad = jnp.sum(pre_grad, axis=0, keepdims=True)
    score_w_grad = jnp.sum(score_grad * hidden, axis=0, keepdims=True)
    start = pl.multiple_of(core_ref[0] * 256, 256)
    for q in range(4):
        columns = slice(EMB * q, EMB * (q + 1))
        keep_ref[256 * q : 256 * (q + 1)] = dense_ref[pl.ds(start, 256), columns]
        send_ref[256 * q : 256 * (q + 1)] = dense_ref[pl.ds(256 - start, 256), columns]
    small = jnp.concatenate(
        [bias_grad[:, EMB * q : EMB * (q + 1)] for q in range(4)]
        + [score_w_grad[:, EMB * q : EMB * (q + 1)] for q in range(4)]
        + [jnp.broadcast_to(loss, (1, EMB))]
        + [jnp.zeros((7, EMB), F32)],
        axis=0,
    )
    keep_ref[1024:] = small
    send_ref[1024:] = small


def back_kernel(pre_grad_ref, slot_ref, slot_col_ref, w_ref, out_ref):
    w_bf = w_ref[...].astype(BF)
    grad = jnp.dot(pre_grad_ref[...], w_bf.T, preferred_element_type=F32).astype(BF).astype(F32)
    slots, slot_cols = slot_ref[...], slot_col_ref[...]
    values, hots = [], []
    for t in range(TABLES):
        which = jnp.broadcast_to(slot_cols[:, t : t + 1] >> 9, (IMPS, EMB))
        values.append(fanned(grad[:, t * EMB : (t + 1) * EMB], which).astype(BF))
        slot = slots[t : t + 1]
        hots.append(hot_cols(slot & 127, (slot >> 7) & 3, 4))
    placed = jnp.dot(
        jnp.concatenate(hots, axis=1), jnp.concatenate(values, axis=0), preferred_element_type=F32
    )
    part = OWNERS // FOLD
    for f in range(FOLD):
        out_ref[f * part : (f + 1) * part] = (
            placed[:, f * EMB : (f + 1) * EMB].astype(BF).reshape(part, LINES, EMB)
        )


def pack_kernel(line_ref, keep_ref, came_ref, out_ref, small_ref):
    out_ref[:, :LINES] = line_ref[...]
    for x in range(4):
        for z in range(8):
            for y in range(4):
                k = 256 * (z % 4) + 8 * (2 * (4 * x + y) + z // 4)
                tile = keep_ref[k : k + 8] + came_ref[k : k + 8]
                high = tile.astype(BF).astype(F32)
                out_ref[(x * 8 + z) * 4 + y, LINES:] = jnp.concatenate(
                    [high, tile - high], axis=0
                ).astype(BF)
    small_ref[...] = keep_ref[1024:] + came_ref[1024:]


def open_kernel(got_ref, small_ref, line_ref, chunk_ref):
    line_ref[...] = got_ref[:, :LINES]
    sums = [jnp.zeros((16, EMB), F32) for _ in range(4)]
    for k in range(OWNERS):
        sums[k % 4] = sums[k % 4] + got_ref[k, LINES:].astype(F32)
    total = (sums[0] + sums[1]) + (sums[2] + sums[3])
    tile = total[:8] + total[8:]
    for k in range(8):
        chunk_ref[k, :8] = tile
        chunk_ref[k, 8:] = small_ref[...]


def column_kernel(got_ref, out_ref):
    small = got_ref[0, 8:]
    for z in range(1, 8):
        small = small + got_ref[z, 8:]
    for p in range(16):
        for z in range(8):
            out_ref[p, 8 * z : 8 * (z + 1)] = got_ref[z, :8]
        out_ref[p, 64:] = small


def place_kernel(
    core_ref, own_ref, other_ref, own_id_ref, other_id_ref, out_ref, wide_ref, buf_ref, sems
):
    core = core_ref[0]
    lines = OWNERS * LINES
    wide_ref[:lines] = own_ref[...].reshape(lines, EMB).astype(F32)
    wide_ref[lines:] = other_ref[...].reshape(lines, EMB).astype(F32)
    cols = [own_id_ref[...], other_id_ref[...]]
    rows = [jnp.transpose(c) for c in cols]
    part = ROWS // 2 // FOLD
    copies = []
    for t in range(TABLES):
        values, hots = [], []
        for s in range(2):
            for r in range(CAP):
                j = CAP * t + r
                line = wide_ref[pl.ds(s * lines + j, OWNERS, stride=LINES), :]
                which = jnp.broadcast_to(cols[s][:, j : j + 1] >> 9, (OWNERS, EMB)) - FOLD * core
                values.append(fanned(line, which).astype(BF))
                row = rows[s][j : j + 1]
                hots.append(hot_cols(row & 127, (row >> 7) & 3, 4))
        total = jnp.dot(
            jnp.concatenate(hots, axis=1), jnp.concatenate(values, axis=0), preferred_element_type=F32
        )
        for f in range(FOLD):
            x = total[:, f * EMB : (f + 1) * EMB]
            mean = jnp.sum(x * x, axis=1, keepdims=True) * (1.0 / EMB)
            buf_ref[t, part * f : part * (f + 1)] = x * (1.0 / (jnp.sqrt(mean) + 1e-06))
        copy = pltpu.make_async_copy(buf_ref.at[t], out_ref.at[t], sems.at[t])
        copy.start()
        copies.append(copy)
    for copy in copies:
        copy.wait()


def final_kernel(core_ref, own_ref, other_ref, w_ref, b_ref, s_ref, loss_ref):
    start = core_ref[0] * 256
    small = own_ref[0, 64:]
    for p in range(1, 16):
        small = small + own_ref[p, 64:]
    kept = small[0:8]
    square = jnp.sum(kept * kept, axis=0, keepdims=True)
    halves = []
    for ref in (own_ref, other_ref):
        sums = [jnp.zeros((8, EMB), F32) for _ in range(4)]
        for p in range(16):
            for z in range(8):
                tile = ref[p, 8 * z : 8 * (z + 1)]
                sums[z % 4] = sums[z % 4] + tile * tile
        halves.append((sums[0] + sums[1]) + (sums[2] + sums[3]))
    main = halves[0] + halves[1]
    square = jnp.sum(square + jnp.sum(main, axis=0, keepdims=True), axis=1, keepdims=True)
    factor = 1.0 / jnp.sqrt(square * (1.0 / (HID * HID + 2 * HID)) + 1e-06)
    for p in range(16):
        for z in range(8):
            row = 8 * (2 * p + z // 4)
            columns = slice(EMB * (z % 4), EMB * (z % 4 + 1))
            w_ref[pl.ds(pl.multiple_of(start + row, 8), 8), columns] = (
                own_ref[p, 8 * z : 8 * (z + 1)] * factor
            )
            w_ref[pl.ds(pl.multiple_of(256 - start + row, 8), 8), columns] = (
                other_ref[p, 8 * z : 8 * (z + 1)] * factor
            )
    b_ref[...] = small[0:4] * factor
    s_ref[...] = small[4:8] * factor
    loss_ref[...] = small[8:9] * (1.0 / 512)


def sds(shape, dtype):
    return jax.ShapeDtypeStruct(shape, dtype)


def call(kernel, mib, outs, ins, scratch=(), out_specs=None, flops=1 << 28):
    return pl.pallas_call(
        kernel,
        out_shape=outs,
        in_specs=ins,
        out_specs=(VMEM,) * len(outs) if out_specs is None else out_specs,
        scratch_shapes=list(scratch),
        cost_estimate=pl.CostEstimate(flops=flops, bytes_accessed=1 << 20, transcendentals=0),
        compiler_params=pltpu.CompilerParams(vmem_limit_bytes=mib << 20),
    )


def exchange(array, axes):
    return lax.all_to_all(array, axes, split_axis=0, concat_axis=0, tiled=True)


def whole_step(
    tables, owner_ids, row_ids, session_of, relevance, logit_bias, w_hidden, bias_hidden, w_score
):
    core = lax.axis_index("dp").astype(jnp.int32).reshape(1)
    swap = [(0, 1), (1, 0)]
    i32 = jnp.int32
    wanted, slots, slot_cols = call(
        slots_kernel, 8,
        (sds((OWNERS, LINES), i32), sds((TABLES, IMPS), i32), sds((IMPS, 2 * TABLES), i32)),
        [HBM, HBM],
        [pltpu.VMEM((8, 128), i32), pltpu.VMEM((TABLES, IMPS), i32), pltpu.SemaphoreType.DMA((2,))],
    )(owner_ids.reshape(8, 128), row_ids.reshape(TABLES, IMPS))
    requested = exchange(wanted, TABLE)
    other_ids = lax.ppermute(requested, "dp", swap)
    (served,) = call(
        serve_kernel, 61,
        (sds((OWNERS, LINES, EMB), BF),),
        [VMEM, HBM],
        [
            pltpu.VMEM((OWNERS * LINES, EMB), F32),
            pltpu.VMEM((TABLES, ROWS, EMB), BF),
            pltpu.SemaphoreType.DMA((TABLES,)),
        ],
    )(requested, tables)
    returned = exchange(served, TABLE)
    half = sds((1024 + SMALL, EMB), F32)
    pre_grad, keep, send = call(
        step_kernel, 24,
        (sds((IMPS, HID), BF), half, half),
        [SMEM] + [VMEM] * 8,
        [pltpu.VMEM((HID, HID), F32)],
    )(
        core, returned, slot_cols, session_of, relevance, logit_bias, w_hidden,
        bias_hidden.reshape(1, HID), w_score.reshape(1, HID),
    )
    came = lax.ppermute(send, "dp", swap)
    (lines,) = call(
        back_kernel, 20, (sds((OWNERS, LINES, EMB), BF),), [VMEM] * 4
    )(pre_grad, slots, slot_cols, w_hidden)
    message, small = call(
        pack_kernel, 12,
        (sds((OWNERS, 2 * LINES, EMB), BF), sds((SMALL, EMB), F32)),
        [VMEM] * 3,
    )(lines, keep, came)
    got = exchange(message, TABLE)
    incoming, chunks = call(
        open_kernel, 12,
        (sds((OWNERS, LINES, EMB), BF), sds((8, 8 + SMALL, EMB), F32)),
        [VMEM] * 2,
    )(got, small)
    other = lax.ppermute(incoming, "dp", swap)
    column = exchange(chunks, "z")
    (emb_step,) = call(
        place_kernel, 28,
        (sds((TABLES, ROWS // 2, EMB), F32),),
        [SMEM] + [VMEM] * 4,
        [
            pltpu.VMEM((2 * OWNERS * LINES, EMB), F32),
            pltpu.VMEM((TABLES, ROWS // 2, EMB), F32),
            pltpu.SemaphoreType.DMA((TABLES,)),
        ],
        out_specs=(ANY,),
    )(core, incoming, other, requested, other_ids)
    (plane,) = call(column_kernel, 12, (sds((16, 64 + SMALL, EMB), F32),), [VMEM])(column)
    mine = exchange(plane, ("x", "y"))
    theirs = lax.ppermute(mine, "dp", swap)
    step_hidden, step_bias, step_score, loss = call(
        final_kernel, 12,
        (sds((HID, HID), F32), sds((4, 128), F32), sds((4, 128), F32), sds((1, 128), F32)),
        [SMEM] + [VMEM] * 2,
    )(core, mine, theirs)
    return emb_step, step_hidden, step_bias.reshape(HID), step_score.reshape(HID), loss[0, 0]


def solution(mesh):
    split = Mesh(mesh.devices.reshape(4, 8, 4, mesh.shape["dp"]), ALL)
    return jax.shard_map(
        whole_step,
        mesh=split,
        in_specs=(
            P(None, TABLE, None),
            P(ALL, None, None, None),
            P(ALL, None, None),
            P(ALL, None),
            P(ALL, None),
            P(ALL, None),
            P(),
            P(),
            P(),
        ),
        out_specs=(P(None, ALL, None), P(), P(), P(), P()),
        check_vma=False,
    )
```

```python
import jax
import jax.numpy as jnp
from jax import lax
from jax.experimental import pallas as pl
from jax.experimental.pallas import tpu as pltpu
from jax.sharding import Mesh
from jax.sharding import PartitionSpec as P


TABLE = ("x", "z", "y")
ALL = ("x", "z", "y", "dp")
TABLES = 4
CAP = 4
LINES = TABLES * CAP
OWNERS = 128
IMPS = 256
EMB = 128
ROWS = 4096
HID = 512
FOLD = 4
SMALL = 16
VMEM = pl.BlockSpec(memory_space=pltpu.VMEM)
ANY = pl.BlockSpec(memory_space=pl.ANY)
BF = jnp.bfloat16
F32 = jnp.float32


HBM = pl.BlockSpec(memory_space=pltpu.HBM)
SMEM = pl.BlockSpec(memory_space=pltpu.SMEM)


def iota(shape, dim):
    return lax.broadcasted_iota(jnp.int32, shape, dim)


def hot_rows(low, block, blocks):
    n = low.shape[0]
    one = jnp.where(iota((n, 128), 1) == low, 1.0, 0.0).astype(BF)
    which = jnp.broadcast_to(block, (n, 128)).astype(F32).astype(BF)
    zero = jnp.zeros((n, 128), BF)
    return jnp.concatenate([jnp.where(which == BF(c), one, zero) for c in range(blocks)], axis=1)


def hot_cols(low, block, blocks):
    n = low.shape[1]
    one = jnp.where(iota((128, n), 0) == low, 1.0, 0.0).astype(BF)
    which = jnp.broadcast_to(block, (128, n)).astype(F32).astype(BF)
    zero = jnp.zeros((128, n), BF)
    return jnp.concatenate([jnp.where(which == BF(c), one, zero) for c in range(blocks)], axis=0)


def chosen(wide, which):
    kept = wide[:, :EMB]
    for f in range(1, FOLD):
        kept = jnp.where(which == f, wide[:, f * EMB : (f + 1) * EMB], kept)
    return kept


def fanned(piece, which):
    zero = jnp.zeros_like(piece)
    return jnp.concatenate([jnp.where(which == f, piece, zero) for f in range(FOLD)], axis=1)


def slots_kernel(core_ref, own_hbm, row_hbm, want_ref, slot_ref, slot_col_ref, own_ref, row_ref, sems):
    copies = [
        pltpu.make_async_copy(own_hbm, own_ref, sems.at[0]),
        pltpu.make_async_copy(row_hbm, row_ref, sems.at[1]),
    ]
    for copy in copies:
        copy.start()
    for copy in copies:
        copy.wait()
    own = own_ref[...]
    own_rows = [
        jnp.concatenate([own[2 * t : 2 * t + 1], own[2 * t + 1 : 2 * t + 2]], axis=1)
        for t in range(TABLES)
    ]
    own_cols = jnp.transpose(jnp.concatenate(own_rows + own_rows, axis=0))
    row_cols = jnp.transpose(jnp.concatenate([row_ref[...], row_ref[...]], axis=0))
    before = iota((IMPS, IMPS), 0) < iota((IMPS, IMPS), 1)
    slots = []
    for t in range(TABLES):
        same = (own_cols[:, t : t + 1] == own_rows[t]) & before
        rank = jnp.sum(jnp.where(same, 1, 0), axis=0, keepdims=True)
        slots.append(own_rows[t] * LINES + (CAP * t) + rank)
    slot_ref[...] = jnp.concatenate(slots, axis=0)
    slot_cols = jnp.transpose(jnp.concatenate(slots + slots, axis=0))
    slot_col_ref[...] = slot_cols
    lines = []
    for t in range(TABLES):
        slot = jnp.broadcast_to(slot_cols[:, t : t + 1], (IMPS, OWNERS))
        row = jnp.broadcast_to(row_cols[:, t : t + 1], (IMPS, OWNERS))
        for r in range(CAP):
            target = iota((IMPS, OWNERS), 1) * LINES + (CAP * t + r)
            lines.append(jnp.sum(jnp.where(slot == target, row, 0), axis=0, keepdims=True))
    want_ref[...] = jnp.transpose(jnp.concatenate(lines, axis=0))


def serve_kernel(req_ref, far_ref, out_ref, wide_ref, tab_ref, sems):
    copies = [pltpu.make_async_copy(far_ref.at[t], tab_ref.at[t], sems.at[t]) for t in range(TABLES)]
    for copy in copies:
        copy.start()
    req = req_ref[...]
    part = ROWS // FOLD
    for t in range(TABLES):
        rows = [req[:, CAP * t + r : CAP * t + r + 1] for r in range(CAP)]
        hot = jnp.concatenate([hot_rows(row & 127, (row >> 7) & 7, 8) for row in rows], axis=0)
        copies[t].wait()
        table = jnp.concatenate(
            [tab_ref[t, f * part : (f + 1) * part, :] for f in range(FOLD)], axis=1
        )
        wide = jnp.dot(hot, table, preferred_element_type=F32)
        for r in range(CAP):
            which = jnp.broadcast_to(rows[r] >> 10, (OWNERS, EMB))
            wide_ref[pl.ds(CAP * t + r, OWNERS, stride=LINES), :] = chosen(
                wide[r * OWNERS : (r + 1) * OWNERS], which
            )
    out_ref[...] = wide_ref[...].astype(BF).reshape(OWNERS, LINES, EMB)


def step_kernel(
    core_ref, ret_ref, slot_col_ref, ses_ref, rel_ref, lb_ref, w_ref, b_ref, ws_ref,
    pre_grad_ref, keep_ref, send_ref, dense_ref,
):
    back = ret_ref[...].reshape(OWNERS * LINES, EMB)
    half = OWNERS * LINES // 2
    source = jnp.concatenate([back[:half], back[half:]], axis=1)
    slot_cols = slot_col_ref[...]
    pieces = []
    for t in range(TABLES):
        slot = slot_cols[:, t : t + 1]
        both = jnp.dot(hot_rows(slot & 127, (slot >> 7) & 7, 8), source, preferred_element_type=F32)
        upper = jnp.broadcast_to(slot, (IMPS, EMB)) >= half
        pieces.append(jnp.where(upper, both[:, EMB:], both[:, :EMB]).astype(BF))
    inputs = jnp.concatenate(pieces, axis=1)
    w_bf = w_ref[...].astype(BF)
    w_score = ws_ref[...]
    pre = jnp.dot(inputs, w_bf, preferred_element_type=F32) + b_ref[...]
    sig = jax.nn.sigmoid(pre)
    hidden = pre * sig
    aux = jnp.transpose(
        jnp.concatenate(
            [rel_ref[...], lb_ref[...], ses_ref[...].astype(F32)] + [rel_ref[...]] * 5, axis=0
        )
    )
    relevance, bias_col, session = aux[:, 0:1], aux[:, 1:2], aux[:, 2:3]
    scores = jnp.sum(hidden * w_score, axis=1, keepdims=True) + bias_col
    first = session < 0.5
    low = jnp.float32(-jnp.inf)
    top = [jnp.max(jnp.where(m, scores, low), axis=0, keepdims=True) for m in (first, ~first)]
    shifted = scores - jnp.where(first, top[0], top[1])
    exponent = jnp.exp(shifted)
    total = [jnp.sum(jnp.where(m, exponent, 0.0), axis=0, keepdims=True) for m in (first, ~first)]
    weight = [jnp.sum(jnp.where(m, relevance, 0.0), axis=0, keepdims=True) for m in (first, ~first)]
    probability = exponent / jnp.where(first, total[0], total[1])
    target = relevance / jnp.where(first, weight[0], weight[1])
    loss = jnp.log(total[0]) + jnp.log(total[1]) - jnp.sum(target * shifted, axis=0, keepdims=True)
    score_grad = probability - target
    pre_grad = score_grad * w_score * (sig * (1.0 + pre * (1.0 - sig)))
    pre_grad_bf = pre_grad.astype(BF)
    pre_grad_ref[...] = pre_grad_bf
    dense_ref[...] = lax.dot_general(
        inputs, pre_grad_bf, (((0,), (0,)), ((), ())), preferred_element_type=F32
    )
    bias_grad = jnp.sum(pre_grad, axis=0, keepdims=True)
    score_w_grad = jnp.sum(score_grad * hidden, axis=0, keepdims=True)
    start = pl.multiple_of(core_ref[0] * 256, 256)
    for q in range(4):
        columns = slice(EMB * q, EMB * (q + 1))
        keep_ref[256 * q : 256 * (q + 1)] = dense_ref[pl.ds(start, 256), columns]
        send_ref[256 * q : 256 * (q + 1)] = dense_ref[pl.ds(256 - start, 256), columns]
    small = jnp.concatenate(
        [bias_grad[:, EMB * q : EMB * (q + 1)] for q in range(4)]
        + [score_w_grad[:, EMB * q : EMB * (q + 1)] for q in range(4)]
        + [jnp.broadcast_to(loss, (1, EMB))]
        + [jnp.zeros((7, EMB), F32)],
        axis=0,
    )
    keep_ref[1024:] = small
    send_ref[1024:] = small


def back_kernel(pre_grad_ref, slot_ref, slot_col_ref, w_ref, out_ref):
    w_bf = w_ref[...].astype(BF)
    grad = jnp.dot(pre_grad_ref[...], w_bf.T, preferred_element_type=F32).astype(BF).astype(F32)
    slots, slot_cols = slot_ref[...], slot_col_ref[...]
    values, hots = [], []
    for t in range(TABLES):
        which = jnp.broadcast_to(slot_cols[:, t : t + 1] >> 9, (IMPS, EMB))
        values.append(fanned(grad[:, t * EMB : (t + 1) * EMB], which).astype(BF))
        slot = slots[t : t + 1]
        hots.append(hot_cols(slot & 127, (slot >> 7) & 3, 4))
    placed = jnp.dot(
        jnp.concatenate(hots, axis=1), jnp.concatenate(values, axis=0), preferred_element_type=F32
    )
    part = OWNERS // FOLD
    for f in range(FOLD):
        out_ref[f * part : (f + 1) * part] = (
            placed[:, f * EMB : (f + 1) * EMB].astype(BF).reshape(part, LINES, EMB)
        )


def pack_kernel(line_ref, keep_ref, came_ref, out_ref, small_ref):
    out_ref[:, :LINES] = line_ref[...]
    for x in range(4):
        for z in range(8):
            for y in range(4):
                k = 256 * (z % 4) + 8 * (2 * (4 * x + y) + z // 4)
                tile = keep_ref[k : k + 8] + came_ref[k : k + 8]
                high = tile.astype(BF).astype(F32)
                out_ref[(x * 8 + z) * 4 + y, LINES:] = jnp.concatenate(
                    [high, tile - high], axis=0
                ).astype(BF)
    small_ref[...] = keep_ref[1024:] + came_ref[1024:]


def open_kernel(got_ref, small_ref, line_ref, chunk_ref):
    line_ref[...] = got_ref[:, :LINES]
    sums = [jnp.zeros((16, EMB), F32) for _ in range(4)]
    for k in range(OWNERS):
        sums[k % 4] = sums[k % 4] + got_ref[k, LINES:].astype(F32)
    total = (sums[0] + sums[1]) + (sums[2] + sums[3])
    tile = total[:8] + total[8:]
    for k in range(8):
        chunk_ref[k, :8] = tile
        chunk_ref[k, 8:] = small_ref[...]


def column_kernel(got_ref, out_ref):
    small = got_ref[0, 8:]
    for z in range(1, 8):
        small = small + got_ref[z, 8:]
    for p in range(16):
        for z in range(8):
            out_ref[p, 8 * z : 8 * (z + 1)] = got_ref[z, :8]
        out_ref[p, 64:] = small


def place_kernel(
    core_ref, own_ref, other_ref, own_id_ref, other_id_ref, out_ref, wide_ref, buf_ref, sems
):
    core = core_ref[0]
    lines = OWNERS * LINES
    wide_ref[:lines] = own_ref[...].reshape(lines, EMB).astype(F32)
    wide_ref[lines:] = other_ref[...].reshape(lines, EMB).astype(F32)
    cols = [own_id_ref[...], other_id_ref[...]]
    rows = [jnp.transpose(c) for c in cols]
    part = ROWS // 2 // FOLD
    copies = []
    for t in range(TABLES):
        values, hots = [], []
        for s in range(2):
            for r in range(CAP):
                j = CAP * t + r
                line = wide_ref[pl.ds(s * lines + j, OWNERS, stride=LINES), :]
                which = jnp.broadcast_to(cols[s][:, j : j + 1] >> 9, (OWNERS, EMB)) - FOLD * core
                values.append(fanned(line, which).astype(BF))
                row = rows[s][j : j + 1]
                hots.append(hot_cols(row & 127, (row >> 7) & 3, 4))
        total = jnp.dot(
            jnp.concatenate(hots, axis=1), jnp.concatenate(values, axis=0), preferred_element_type=F32
        )
        for f in range(FOLD):
            x = total[:, f * EMB : (f + 1) * EMB]
            mean = jnp.sum(x * x, axis=1, keepdims=True) * (1.0 / EMB)
            buf_ref[t, part * f : part * (f + 1)] = x * (1.0 / (jnp.sqrt(mean) + 1e-06))
        copy = pltpu.make_async_copy(buf_ref.at[t], out_ref.at[t], sems.at[t])
        copy.start()
        copies.append(copy)
    for copy in copies:
        copy.wait()


def final_kernel(core_ref, own_ref, other_ref, w_ref, b_ref, s_ref, loss_ref):
    start = core_ref[0] * 256
    small = own_ref[0, 64:]
    for p in range(1, 16):
        small = small + own_ref[p, 64:]
    kept = small[0:8]
    square = jnp.sum(kept * kept, axis=0, keepdims=True)
    halves = []
    for ref in (own_ref, other_ref):
        sums = [jnp.zeros((8, EMB), F32) for _ in range(4)]
        for p in range(16):
            for z in range(8):
                tile = ref[p, 8 * z : 8 * (z + 1)]
                sums[z % 4] = sums[z % 4] + tile * tile
        halves.append((sums[0] + sums[1]) + (sums[2] + sums[3]))
    main = halves[0] + halves[1]
    square = jnp.sum(square + jnp.sum(main, axis=0, keepdims=True), axis=1, keepdims=True)
    factor = 1.0 / jnp.sqrt(square * (1.0 / (HID * HID + 2 * HID)) + 1e-06)
    for p in range(16):
        for z in range(8):
            row = 8 * (2 * p + z // 4)
            columns = slice(EMB * (z % 4), EMB * (z % 4 + 1))
            w_ref[pl.ds(pl.multiple_of(start + row, 8), 8), columns] = (
                own_ref[p, 8 * z : 8 * (z + 1)] * factor
            )
            w_ref[pl.ds(pl.multiple_of(256 - start + row, 8), 8), columns] = (
                other_ref[p, 8 * z : 8 * (z + 1)] * factor
            )
    b_ref[...] = small[0:4] * factor
    s_ref[...] = small[4:8] * factor
    loss_ref[...] = small[8:9] * (1.0 / 512)


def sds(shape, dtype):
    return jax.ShapeDtypeStruct(shape, dtype)


def call(kernel, mib, outs, ins, scratch=(), out_specs=None, flops=1 << 28):
    return pl.pallas_call(
        kernel,
        out_shape=outs,
        in_specs=ins,
        out_specs=(VMEM,) * len(outs) if out_specs is None else out_specs,
        scratch_shapes=list(scratch),
        cost_estimate=pl.CostEstimate(flops=flops, bytes_accessed=1 << 20, transcendentals=0),
        compiler_params=pltpu.CompilerParams(vmem_limit_bytes=mib << 20),
    )


def exchange(array, axes):
    return lax.all_to_all(array, axes, split_axis=0, concat_axis=0, tiled=True)


def whole_step(
    tables, owner_ids, row_ids, session_of, relevance, logit_bias, w_hidden, bias_hidden, w_score
):
    core = lax.axis_index("dp").astype(jnp.int32).reshape(1)
    swap = [(0, 1), (1, 0)]
    i32 = jnp.int32
    wanted, slots, slot_cols = call(
        slots_kernel, 8,
        (sds((OWNERS, LINES), i32), sds((TABLES, IMPS), i32), sds((IMPS, 2 * TABLES), i32)),
        [SMEM, HBM, HBM],
        [pltpu.VMEM((8, 128), i32), pltpu.VMEM((TABLES, IMPS), i32), pltpu.SemaphoreType.DMA((2,))],
    )(
        core,
        pltpu.with_memory_space_constraint(owner_ids.reshape(8, 128), pltpu.HBM),
        pltpu.with_memory_space_constraint(row_ids.reshape(TABLES, IMPS), pltpu.HBM),
    )
    requested = exchange(wanted, TABLE)
    other_ids = lax.ppermute(requested, "dp", swap)
    (served,) = call(
        serve_kernel, 24,
        (sds((OWNERS, LINES, EMB), BF),),
        [VMEM, HBM],
        [
            pltpu.VMEM((OWNERS * LINES, EMB), F32),
            pltpu.VMEM((TABLES, ROWS, EMB), BF),
            pltpu.SemaphoreType.DMA((TABLES,)),
        ],
    )(requested, pltpu.with_memory_space_constraint(tables, pltpu.HBM))
    returned = exchange(served, TABLE)
    half = sds((1024 + SMALL, EMB), F32)
    pre_grad, keep, send = call(
        step_kernel, 24,
        (sds((IMPS, HID), BF), half, half),
        [SMEM] + [VMEM] * 8,
        [pltpu.VMEM((HID, HID), F32)],
    )(
        core, returned, slot_cols, session_of, relevance, logit_bias, w_hidden,
        bias_hidden.reshape(1, HID), w_score.reshape(1, HID),
    )
    came = lax.ppermute(send, "dp", swap)
    (lines,) = call(
        back_kernel, 20, (sds((OWNERS, LINES, EMB), BF),), [VMEM] * 4
    )(pre_grad, slots, slot_cols, w_hidden)
    message, small = call(
        pack_kernel, 12,
        (sds((OWNERS, 2 * LINES, EMB), BF), sds((SMALL, EMB), F32)),
        [VMEM] * 3,
    )(lines, keep, came)
    got = exchange(message, TABLE)
    incoming, chunks = call(
        open_kernel, 12,
        (sds((OWNERS, LINES, EMB), BF), sds((8, 8 + SMALL, EMB), F32)),
        [VMEM] * 2,
    )(got, small)
    other = lax.ppermute(incoming, "dp", swap)
    column = exchange(chunks, "z")
    (emb_step,) = call(
        place_kernel, 28,
        (sds((TABLES, ROWS // 2, EMB), F32),),
        [SMEM] + [VMEM] * 4,
        [
            pltpu.VMEM((2 * OWNERS * LINES, EMB), F32),
            pltpu.VMEM((TABLES, ROWS // 2, EMB), F32),
            pltpu.SemaphoreType.DMA((TABLES,)),
        ],
        out_specs=(ANY,),
    )(core, incoming, other, requested, other_ids)
    (plane,) = call(column_kernel, 12, (sds((16, 64 + SMALL, EMB), F32),), [VMEM])(column)
    mine = exchange(plane, ("x", "y"))
    theirs = lax.ppermute(mine, "dp", swap)
    step_hidden, step_bias, step_score, loss = call(
        final_kernel, 12,
        (sds((HID, HID), F32), sds((4, 128), F32), sds((4, 128), F32), sds((1, 128), F32)),
        [SMEM] + [VMEM] * 2,
    )(core, mine, theirs)
    return emb_step, step_hidden, step_bias.reshape(HID), step_score.reshape(HID), loss[0, 0]


def solution(mesh):
    split = Mesh(mesh.devices.reshape(4, 8, 4, mesh.shape["dp"]), ALL)
    return jax.shard_map(
        whole_step,
        mesh=split,
        in_specs=(
            P(None, TABLE, None),
            P(ALL, None, None, None),
            P(ALL, None, None),
            P(ALL, None),
            P(ALL, None),
            P(ALL, None),
            P(),
            P(),
            P(),
        ),
        out_specs=(P(None, ALL, None), P(), P(), P(), P()),
        check_vma=False,
    )
```

```python
import jax
import jax.numpy as jnp
from jax import lax
from jax.experimental import pallas as pl
from jax.experimental.pallas import tpu as pltpu
from jax.sharding import Mesh
from jax.sharding import PartitionSpec as P


TABLE = ("x", "z", "y")
ALL = ("x", "z", "y", "dp")
TABLES = 4
CAP = 4
LINES = TABLES * CAP
OWNERS = 128
IMPS = 256
EMB = 128
ROWS = 4096
HID = 512
FOLD = 4
SMALL = 16
VMEM = pl.BlockSpec(memory_space=pltpu.VMEM)
ANY = pl.BlockSpec(memory_space=pl.ANY)
BF = jnp.bfloat16
F32 = jnp.float32


HBM = pl.BlockSpec(memory_space=pltpu.HBM)
SMEM = pl.BlockSpec(memory_space=pltpu.SMEM)


def iota(shape, dim):
    return lax.broadcasted_iota(jnp.int32, shape, dim)


def hot_rows(low, block, blocks):
    n = low.shape[0]
    one = jnp.where(iota((n, 128), 1) == low, 1.0, 0.0).astype(BF)
    which = jnp.broadcast_to(block, (n, 128)).astype(F32).astype(BF)
    zero = jnp.zeros((n, 128), BF)
    return jnp.concatenate([jnp.where(which == BF(c), one, zero) for c in range(blocks)], axis=1)


def hot_cols(low, block, blocks):
    n = low.shape[1]
    one = jnp.where(iota((128, n), 0) == low, 1.0, 0.0).astype(BF)
    which = jnp.broadcast_to(block, (128, n)).astype(F32).astype(BF)
    zero = jnp.zeros((128, n), BF)
    return jnp.concatenate([jnp.where(which == BF(c), one, zero) for c in range(blocks)], axis=0)


def chosen(wide, which):
    kept = wide[:, :EMB]
    for f in range(1, FOLD):
        kept = jnp.where(which == f, wide[:, f * EMB : (f + 1) * EMB], kept)
    return kept


def fanned(piece, which):
    zero = jnp.zeros_like(piece)
    return jnp.concatenate([jnp.where(which == f, piece, zero) for f in range(FOLD)], axis=1)


def slots_kernel(core_ref, own_hbm, row_hbm, want_ref, slot_ref, slot_col_ref, own_ref, row_ref, sems):
    copies = [
        pltpu.make_async_copy(own_hbm, own_ref, sems.at[0]),
        pltpu.make_async_copy(row_hbm, row_ref, sems.at[1]),
    ]
    for copy in copies:
        copy.start()
    for copy in copies:
        copy.wait()
    own = own_ref[...]
    own_rows = [
        jnp.concatenate([own[2 * t : 2 * t + 1], own[2 * t + 1 : 2 * t + 2]], axis=1)
        for t in range(TABLES)
    ]
    own_cols = jnp.transpose(jnp.concatenate(own_rows + own_rows, axis=0))
    row_cols = jnp.transpose(jnp.concatenate([row_ref[...], row_ref[...]], axis=0))
    before = iota((IMPS, IMPS), 0) < iota((IMPS, IMPS), 1)
    slots = []
    for t in range(TABLES):
        same = (own_cols[:, t : t + 1] == own_rows[t]) & before
        rank = jnp.sum(jnp.where(same, 1, 0), axis=0, keepdims=True)
        slots.append(own_rows[t] * LINES + (CAP * t) + rank)
    slot_ref[...] = jnp.concatenate(slots, axis=0)
    slot_cols = jnp.transpose(jnp.concatenate(slots + slots, axis=0))
    slot_col_ref[...] = slot_cols
    lines = []
    for t in range(TABLES):
        slot = jnp.broadcast_to(slot_cols[:, t : t + 1], (IMPS, OWNERS))
        row = jnp.broadcast_to(row_cols[:, t : t + 1], (IMPS, OWNERS))
        for r in range(CAP):
            target = iota((IMPS, OWNERS), 1) * LINES + (CAP * t + r)
            lines.append(jnp.sum(jnp.where(slot == target, row, 0), axis=0, keepdims=True))
    want_ref[...] = jnp.transpose(jnp.concatenate(lines, axis=0))


def serve_kernel(req_ref, far_ref, out_ref, wide_ref, tab_ref, sems):
    copies = [pltpu.make_async_copy(far_ref.at[t], tab_ref.at[t], sems.at[t]) for t in range(TABLES)]
    for copy in copies:
        copy.start()
    req = req_ref[...]
    part = ROWS // FOLD
    for t in range(TABLES):
        rows = [req[:, CAP * t + r : CAP * t + r + 1] for r in range(CAP)]
        hot = jnp.concatenate([hot_rows(row & 127, (row >> 7) & 7, 8) for row in rows], axis=0)
        copies[t].wait()
        table = jnp.concatenate(
            [tab_ref[t, f * part : (f + 1) * part, :] for f in range(FOLD)], axis=1
        )
        wide = jnp.dot(hot, table, preferred_element_type=F32)
        for r in range(CAP):
            which = jnp.broadcast_to(rows[r] >> 10, (OWNERS, EMB))
            wide_ref[pl.ds(CAP * t + r, OWNERS, stride=LINES), :] = chosen(
                wide[r * OWNERS : (r + 1) * OWNERS], which
            )
    out_ref[...] = wide_ref[...].astype(BF).reshape(OWNERS, LINES, EMB)


def step_kernel(
    core_ref, ret_ref, slot_col_ref, ses_ref, rel_ref, lb_ref, w_ref, b_ref, ws_ref,
    pre_grad_ref, keep_ref, send_ref, dense_ref,
):
    back = ret_ref[...].reshape(OWNERS * LINES, EMB)
    half = OWNERS * LINES // 2
    source = jnp.concatenate([back[:half], back[half:]], axis=1)
    slot_cols = slot_col_ref[...]
    pieces = []
    for t in range(TABLES):
        slot = slot_cols[:, t : t + 1]
        both = jnp.dot(hot_rows(slot & 127, (slot >> 7) & 7, 8), source, preferred_element_type=F32)
        upper = jnp.broadcast_to(slot, (IMPS, EMB)) >= half
        pieces.append(jnp.where(upper, both[:, EMB:], both[:, :EMB]).astype(BF))
    inputs = jnp.concatenate(pieces, axis=1)
    w_bf = w_ref[...].astype(BF)
    w_score = ws_ref[...]
    pre = jnp.dot(inputs, w_bf, preferred_element_type=F32) + b_ref[...]
    sig = jax.nn.sigmoid(pre)
    hidden = pre * sig
    aux = jnp.transpose(
        jnp.concatenate(
            [rel_ref[...], lb_ref[...], ses_ref[...].astype(F32)] + [rel_ref[...]] * 5, axis=0
        )
    )
    relevance, bias_col, session = aux[:, 0:1], aux[:, 1:2], aux[:, 2:3]
    scores = jnp.sum(hidden * w_score, axis=1, keepdims=True) + bias_col
    first = session < 0.5
    low = jnp.float32(-jnp.inf)
    top = [jnp.max(jnp.where(m, scores, low), axis=0, keepdims=True) for m in (first, ~first)]
    shifted = scores - jnp.where(first, top[0], top[1])
    exponent = jnp.exp(shifted)
    total = [jnp.sum(jnp.where(m, exponent, 0.0), axis=0, keepdims=True) for m in (first, ~first)]
    weight = [jnp.sum(jnp.where(m, relevance, 0.0), axis=0, keepdims=True) for m in (first, ~first)]
    probability = exponent / jnp.where(first, total[0], total[1])
    target = relevance / jnp.where(first, weight[0], weight[1])
    loss = jnp.log(total[0]) + jnp.log(total[1]) - jnp.sum(target * shifted, axis=0, keepdims=True)
    score_grad = probability - target
    pre_grad = score_grad * w_score * (sig * (1.0 + pre * (1.0 - sig)))
    pre_grad_bf = pre_grad.astype(BF)
    pre_grad_ref[...] = pre_grad_bf
    dense_ref[...] = lax.dot_general(
        inputs, pre_grad_bf, (((0,), (0,)), ((), ())), preferred_element_type=F32
    )
    bias_grad = jnp.sum(pre_grad, axis=0, keepdims=True)
    score_w_grad = jnp.sum(score_grad * hidden, axis=0, keepdims=True)
    start = pl.multiple_of(core_ref[0] * 256, 256)
    for y in range(4):
        for x in range(4):
            for z in range(8):
                k = ((y * 4 + x) * 8 + z) * 8
                row, columns = 8 * (2 * (4 * x + y) + z // 4), slice(EMB * (z % 4), EMB * (z % 4 + 1))
                for ref, base in ((keep_ref, start), (send_ref, 256 - start)):
                    ref[k : k + 8] = dense_ref[pl.ds(pl.multiple_of(base + row, 8), 8), columns]
    small = jnp.concatenate(
        [bias_grad[:, EMB * q : EMB * (q + 1)] for q in range(4)]
        + [score_w_grad[:, EMB * q : EMB * (q + 1)] for q in range(4)]
        + [jnp.broadcast_to(loss, (1, EMB))]
        + [jnp.zeros((7, EMB), F32)],
        axis=0,
    )
    keep_ref[1024:] = small
    send_ref[1024:] = small


def back_kernel(pre_grad_ref, slot_ref, slot_col_ref, w_ref, out_ref):
    w_bf = w_ref[...].astype(BF)
    grad = jnp.dot(pre_grad_ref[...], w_bf.T, preferred_element_type=F32).astype(BF).astype(F32)
    slots, slot_cols = slot_ref[...], slot_col_ref[...]
    values, hots = [], []
    for t in range(TABLES):
        which = jnp.broadcast_to(slot_cols[:, t : t + 1] >> 9, (IMPS, EMB))
        values.append(fanned(grad[:, t * EMB : (t + 1) * EMB], which).astype(BF))
        slot = slots[t : t + 1]
        hots.append(hot_cols(slot & 127, (slot >> 7) & 3, 4))
    placed = jnp.dot(
        jnp.concatenate(hots, axis=1), jnp.concatenate(values, axis=0), preferred_element_type=F32
    )
    part = OWNERS // FOLD
    for f in range(FOLD):
        out_ref[f * part : (f + 1) * part] = (
            placed[:, f * EMB : (f + 1) * EMB].astype(BF).reshape(part, LINES, EMB)
        )


def chip_kernel(at_ref, keep_ref, came_ref, own_ref, one_ref, two_ref, three_ref, small_ref, sum_ref):
    sum_ref[...] = keep_ref[:1024] + came_ref[:1024]
    small_ref[...] = keep_ref[1024:] + came_ref[1024:]
    for d, ref in enumerate((own_ref, one_ref, two_ref, three_ref)):
        ref[...] = sum_ref[pl.ds(pl.multiple_of(((at_ref[0] + d) & 3) * 256, 256), 256), :]


def cross_kernel(
    at_ref, mine_ref, a_ref, b_ref, c_ref, own_ref, one_ref, two_ref, three_ref, sum_ref
):
    sum_ref[...] = (mine_ref[...] + a_ref[...]) + (b_ref[...] + c_ref[...])
    for d, ref in enumerate((own_ref, one_ref, two_ref, three_ref)):
        ref[...] = sum_ref[pl.ds(pl.multiple_of(((at_ref[0] + d) & 3) * 64, 64), 64), :]


def plane_kernel(mine_ref, a_ref, b_ref, c_ref, small_ref, out_ref):
    total = (mine_ref[...] + a_ref[...]) + (b_ref[...] + c_ref[...])
    small = small_ref[...]
    for k in range(8):
        out_ref[k, :64] = total
        out_ref[k, 64:] = small


def column_kernel(got_ref, out_ref):
    total = got_ref[0]
    for z in range(1, 8):
        total = total + got_ref[z]
    for p in range(16):
        out_ref[p] = total


def place_kernel(
    core_ref, own_ref, other_ref, own_id_ref, other_id_ref, out_ref, wide_ref, buf_ref, sems
):
    core = core_ref[0]
    lines = OWNERS * LINES
    wide_ref[:lines] = own_ref[...].reshape(lines, EMB).astype(F32)
    wide_ref[lines:] = other_ref[...].reshape(lines, EMB).astype(F32)
    cols = [own_id_ref[...], other_id_ref[...]]
    rows = [jnp.transpose(c) for c in cols]
    part = ROWS // 2 // FOLD
    copies = []
    for t in range(TABLES):
        values, hots = [], []
        for s in range(2):
            for r in range(CAP):
                j = CAP * t + r
                line = wide_ref[pl.ds(s * lines + j, OWNERS, stride=LINES), :]
                which = jnp.broadcast_to(cols[s][:, j : j + 1] >> 9, (OWNERS, EMB)) - FOLD * core
                values.append(fanned(line, which).astype(BF))
                row = rows[s][j : j + 1]
                hots.append(hot_cols(row & 127, (row >> 7) & 3, 4))
        total = jnp.dot(
            jnp.concatenate(hots, axis=1), jnp.concatenate(values, axis=0), preferred_element_type=F32
        )
        for f in range(FOLD):
            x = total[:, f * EMB : (f + 1) * EMB]
            mean = jnp.sum(x * x, axis=1, keepdims=True) * (1.0 / EMB)
            buf_ref[t, part * f : part * (f + 1)] = x * (1.0 / (jnp.sqrt(mean) + 1e-06))
        copy = pltpu.make_async_copy(buf_ref.at[t], out_ref.at[t], sems.at[t])
        copy.start()
        copies.append(copy)
    for copy in copies:
        copy.wait()


def final_kernel(core_ref, own_ref, other_ref, w_ref, b_ref, s_ref, loss_ref):
    start = core_ref[0] * 256
    small = own_ref[0, 64:]
    for p in range(1, 16):
        small = small + own_ref[p, 64:]
    kept = small[0:8]
    square = jnp.sum(kept * kept, axis=0, keepdims=True)
    halves = []
    for ref in (own_ref, other_ref):
        sums = [jnp.zeros((8, EMB), F32) for _ in range(4)]
        for p in range(16):
            for z in range(8):
                tile = ref[p, 8 * z : 8 * (z + 1)]
                sums[z % 4] = sums[z % 4] + tile * tile
        halves.append((sums[0] + sums[1]) + (sums[2] + sums[3]))
    main = halves[0] + halves[1]
    square = jnp.sum(square + jnp.sum(main, axis=0, keepdims=True), axis=1, keepdims=True)
    factor = 1.0 / jnp.sqrt(square * (1.0 / (HID * HID + 2 * HID)) + 1e-06)
    for p in range(16):
        for z in range(8):
            row = 8 * (2 * p + z // 4)
            columns = slice(EMB * (z % 4), EMB * (z % 4 + 1))
            w_ref[pl.ds(pl.multiple_of(start + row, 8), 8), columns] = (
                own_ref[p, 8 * z : 8 * (z + 1)] * factor
            )
            w_ref[pl.ds(pl.multiple_of(256 - start + row, 8), 8), columns] = (
                other_ref[p, 8 * z : 8 * (z + 1)] * factor
            )
    b_ref[...] = small[0:4] * factor
    s_ref[...] = small[4:8] * factor
    loss_ref[...] = small[8:9] * (1.0 / 512)


def sds(shape, dtype):
    return jax.ShapeDtypeStruct(shape, dtype)


def call(kernel, mib, outs, ins, scratch=(), out_specs=None, flops=1 << 28):
    return pl.pallas_call(
        kernel,
        out_shape=outs,
        in_specs=ins,
        out_specs=(VMEM,) * len(outs) if out_specs is None else out_specs,
        scratch_shapes=list(scratch),
        cost_estimate=pl.CostEstimate(flops=flops, bytes_accessed=1 << 20, transcendentals=0),
        compiler_params=pltpu.CompilerParams(vmem_limit_bytes=mib << 20),
    )


def exchange(array, axes):
    return lax.all_to_all(array, axes, split_axis=0, concat_axis=0, tiled=True)


def whole_step(
    tables, owner_ids, row_ids, session_of, relevance, logit_bias, w_hidden, bias_hidden, w_score
):
    core = lax.axis_index("dp").astype(jnp.int32).reshape(1)
    swap = [(0, 1), (1, 0)]
    i32 = jnp.int32
    wanted, slots, slot_cols = call(
        slots_kernel, 8,
        (sds((OWNERS, LINES), i32), sds((TABLES, IMPS), i32), sds((IMPS, 2 * TABLES), i32)),
        [SMEM, HBM, HBM],
        [pltpu.VMEM((8, 128), i32), pltpu.VMEM((TABLES, IMPS), i32), pltpu.SemaphoreType.DMA((2,))],
    )(
        core,
        pltpu.with_memory_space_constraint(owner_ids.reshape(8, 128), pltpu.HBM),
        pltpu.with_memory_space_constraint(row_ids.reshape(TABLES, IMPS), pltpu.HBM),
    )
    requested = exchange(wanted, TABLE)
    other_ids = lax.ppermute(requested, "dp", swap)
    (served,) = call(
        serve_kernel, 24,
        (sds((OWNERS, LINES, EMB), BF),),
        [VMEM, HBM],
        [
            pltpu.VMEM((OWNERS * LINES, EMB), F32),
            pltpu.VMEM((TABLES, ROWS, EMB), BF),
            pltpu.SemaphoreType.DMA((TABLES,)),
        ],
    )(requested, pltpu.with_memory_space_constraint(tables, pltpu.HBM))
    returned = exchange(served, TABLE)
    half = sds((1024 + SMALL, EMB), F32)
    pre_grad, keep, send = call(
        step_kernel, 24,
        (sds((IMPS, HID), BF), half, half),
        [SMEM] + [VMEM] * 8,
        [pltpu.VMEM((HID, HID), F32)],
    )(
        core, returned, slot_cols, session_of, relevance, logit_bias, w_hidden,
        bias_hidden.reshape(1, HID), w_score.reshape(1, HID),
    )
    came = lax.ppermute(send, "dp", swap)
    (lines,) = call(
        back_kernel, 20, (sds((OWNERS, LINES, EMB), BF),), [VMEM] * 4
    )(pre_grad, slots, slot_cols, w_hidden)
    incoming = exchange(lines, TABLE)

    def spread(parts, axis):
        return [
            lax.ppermute(part, axis, [(i, (i + d) % 4) for i in range(4)])
            for d, part in enumerate(parts, 1)
        ]

    quarter, tiles = sds((256, EMB), F32), sds((64, EMB), F32)
    own, *rest, small = call(
        chip_kernel, 12, (quarter,) * 4 + (sds((SMALL, EMB), F32),), [SMEM] + [VMEM] * 2,
        [pltpu.VMEM((1024, EMB), F32)],
    )(lax.axis_index("y").astype(i32).reshape(1), keep, came)
    rest = spread(rest, "y")
    own, *rest = call(
        cross_kernel, 12, (tiles,) * 4, [SMEM] + [VMEM] * 4,
        [pltpu.VMEM((256, EMB), F32)],
    )(lax.axis_index("x").astype(i32).reshape(1), own, *rest)
    rest = spread(rest, "x")
    (chunks,) = call(
        plane_kernel, 12, (sds((8, 64 + SMALL, EMB), F32),), [VMEM] * 5
    )(own, *rest, small)
    other = lax.ppermute(incoming, "dp", swap)
    column = exchange(chunks, "z")
    (emb_step,) = call(
        place_kernel, 28,
        (sds((TABLES, ROWS // 2, EMB), F32),),
        [SMEM] + [VMEM] * 4,
        [
            pltpu.VMEM((2 * OWNERS * LINES, EMB), F32),
            pltpu.VMEM((TABLES, ROWS // 2, EMB), F32),
            pltpu.SemaphoreType.DMA((TABLES,)),
        ],
        out_specs=(ANY,),
    )(core, incoming, other, requested, other_ids)
    (sums,) = call(column_kernel, 12, (sds((16, 64 + SMALL, EMB), F32),), [VMEM])(column)
    mine = exchange(sums, ("x", "y"))
    theirs = lax.ppermute(mine, "dp", swap)
    step_hidden, step_bias, step_score, loss = call(
        final_kernel, 12,
        (sds((HID, HID), F32), sds((4, 128), F32), sds((4, 128), F32), sds((1, 128), F32)),
        [SMEM] + [VMEM] * 2,
    )(core, mine, theirs)
    return emb_step, step_hidden, step_bias.reshape(HID), step_score.reshape(HID), loss[0, 0]


def solution(mesh):
    split = Mesh(mesh.devices.reshape(4, 8, 4, mesh.shape["dp"]), ALL)
    return jax.shard_map(
        whole_step,
        mesh=split,
        in_specs=(
            P(None, TABLE, None),
            P(ALL, None, None, None),
            P(ALL, None, None),
            P(ALL, None),
            P(ALL, None),
            P(ALL, None),
            P(),
            P(),
            P(),
        ),
        out_specs=(P(None, ALL, None), P(), P(), P(), P()),
        check_vma=False,
    )
```

```python
import jax
import jax.numpy as jnp
from jax import lax
from jax.experimental import pallas as pl
from jax.experimental.pallas import tpu as pltpu
from jax.sharding import Mesh
from jax.sharding import PartitionSpec as P


TABLE = ("x", "z", "y")
ALL = ("x", "z", "y", "dp")
TABLES = 4
CAP = 4
LINES = TABLES * CAP
OWNERS = 128
IMPS = 256
EMB = 128
ROWS = 4096
HID = 512
FOLD = 4
SMALL = 8
VMEM = pl.BlockSpec(memory_space=pltpu.VMEM)
ANY = pl.BlockSpec(memory_space=pl.ANY)
BF = jnp.bfloat16
F32 = jnp.float32


HBM = pl.BlockSpec(memory_space=pltpu.HBM)
SMEM = pl.BlockSpec(memory_space=pltpu.SMEM)


def iota(shape, dim):
    return lax.broadcasted_iota(jnp.int32, shape, dim)


def hot_rows(low, block, blocks):
    n = low.shape[0]
    one = jnp.where(iota((n, 128), 1) == low, 1.0, 0.0).astype(BF)
    which = jnp.broadcast_to(block, (n, 128)).astype(F32).astype(BF)
    zero = jnp.zeros((n, 128), BF)
    return jnp.concatenate([jnp.where(which == BF(c), one, zero) for c in range(blocks)], axis=1)


def hot_cols(low, block, blocks):
    n = low.shape[1]
    one = jnp.where(iota((128, n), 0) == low, 1.0, 0.0).astype(BF)
    which = jnp.broadcast_to(block, (128, n)).astype(F32).astype(BF)
    zero = jnp.zeros((128, n), BF)
    return jnp.concatenate([jnp.where(which == BF(c), one, zero) for c in range(blocks)], axis=0)


def chosen(wide, which):
    kept = wide[:, :EMB]
    for f in range(1, FOLD):
        kept = jnp.where(which == f, wide[:, f * EMB : (f + 1) * EMB], kept)
    return kept


def fanned(piece, which):
    zero = jnp.zeros_like(piece)
    return jnp.concatenate([jnp.where(which == f, piece, zero) for f in range(FOLD)], axis=1)


def slots_kernel(core_ref, own_hbm, row_hbm, want_ref, slot_ref, slot_col_ref, own_ref, row_ref, sems):
    copies = [
        pltpu.make_async_copy(own_hbm, own_ref, sems.at[0]),
        pltpu.make_async_copy(row_hbm, row_ref, sems.at[1]),
    ]
    for copy in copies:
        copy.start()
    for copy in copies:
        copy.wait()
    own = own_ref[...]
    own_rows = [
        jnp.concatenate([own[2 * t : 2 * t + 1], own[2 * t + 1 : 2 * t + 2]], axis=1)
        for t in range(TABLES)
    ]
    own_cols = jnp.transpose(jnp.concatenate(own_rows + own_rows, axis=0))
    row_cols = jnp.transpose(jnp.concatenate([row_ref[...], row_ref[...]], axis=0))
    before = iota((IMPS, IMPS), 0) < iota((IMPS, IMPS), 1)
    slots = []
    for t in range(TABLES):
        same = (own_cols[:, t : t + 1] == own_rows[t]) & before
        rank = jnp.sum(jnp.where(same, 1, 0), axis=0, keepdims=True)
        slots.append(own_rows[t] * LINES + (CAP * t) + rank)
    slot_ref[...] = jnp.concatenate(slots, axis=0)
    slot_cols = jnp.transpose(jnp.concatenate(slots + slots, axis=0))
    slot_col_ref[...] = slot_cols
    lines = []
    for t in range(TABLES):
        slot = jnp.broadcast_to(slot_cols[:, t : t + 1], (IMPS, OWNERS))
        row = jnp.broadcast_to(row_cols[:, t : t + 1], (IMPS, OWNERS))
        for r in range(CAP):
            target = iota((IMPS, OWNERS), 1) * LINES + (CAP * t + r)
            lines.append(jnp.sum(jnp.where(slot == target, row, 0), axis=0, keepdims=True))
    want_ref[...] = jnp.transpose(jnp.concatenate(lines, axis=0))


def serve_kernel(req_ref, far_ref, out_ref, wide_ref, tab_ref, sems):
    copies = [pltpu.make_async_copy(far_ref.at[t], tab_ref.at[t], sems.at[t]) for t in range(TABLES)]
    for copy in copies:
        copy.start()
    req = req_ref[...]
    part = ROWS // FOLD
    for t in range(TABLES):
        rows = [req[:, CAP * t + r : CAP * t + r + 1] for r in range(CAP)]
        hot = jnp.concatenate([hot_rows(row & 127, (row >> 7) & 7, 8) for row in rows], axis=0)
        copies[t].wait()
        table = jnp.concatenate(
            [tab_ref[t, f * part : (f + 1) * part, :] for f in range(FOLD)], axis=1
        )
        wide = jnp.dot(hot, table, preferred_element_type=F32)
        for r in range(CAP):
            which = jnp.broadcast_to(rows[r] >> 10, (OWNERS, EMB))
            wide_ref[pl.ds(CAP * t + r, OWNERS, stride=LINES), :] = chosen(
                wide[r * OWNERS : (r + 1) * OWNERS], which
            )
    out_ref[...] = wide_ref[...].astype(BF).reshape(OWNERS, LINES, EMB)


def step_kernel(
    core_ref, ret_ref, slot_col_ref, ses_ref, rel_ref, lb_ref, w_ref, b_ref, ws_ref,
    pre_grad_ref, keep_ref, send_ref, dense_ref,
):
    back = ret_ref[...].reshape(OWNERS * LINES, EMB)
    half = OWNERS * LINES // 2
    source = jnp.concatenate([back[:half], back[half:]], axis=1)
    slot_cols = slot_col_ref[...]
    pieces = []
    for t in range(TABLES):
        slot = slot_cols[:, t : t + 1]
        both = jnp.dot(hot_rows(slot & 127, (slot >> 7) & 7, 8), source, preferred_element_type=F32)
        upper = jnp.broadcast_to(slot, (IMPS, EMB)) >= half
        pieces.append(jnp.where(upper, both[:, EMB:], both[:, :EMB]).astype(BF))
    inputs = jnp.concatenate(pieces, axis=1)
    w_bf = w_ref[...].astype(BF)
    w_score = ws_ref[...]
    pre = jnp.dot(inputs, w_bf, preferred_element_type=F32) + b_ref[...]
    sig = jax.nn.sigmoid(pre)
    hidden = pre * sig
    aux = jnp.transpose(
        jnp.concatenate(
            [rel_ref[...], lb_ref[...], ses_ref[...].astype(F32)] + [rel_ref[...]] * 5, axis=0
        )
    )
    relevance, bias_col, session = aux[:, 0:1], aux[:, 1:2], aux[:, 2:3]
    scores = jnp.sum(hidden * w_score, axis=1, keepdims=True) + bias_col
    first = session < 0.5
    low = jnp.float32(-jnp.inf)
    top = [jnp.max(jnp.where(m, scores, low), axis=0, keepdims=True) for m in (first, ~first)]
    shifted = scores - jnp.where(first, top[0], top[1])
    exponent = jnp.exp(shifted)
    total = [jnp.sum(jnp.where(m, exponent, 0.0), axis=0, keepdims=True) for m in (first, ~first)]
    weight = [jnp.sum(jnp.where(m, relevance, 0.0), axis=0, keepdims=True) for m in (first, ~first)]
    probability = exponent / jnp.where(first, total[0], total[1])
    target = relevance / jnp.where(first, weight[0], weight[1])
    loss = jnp.log(total[0]) + jnp.log(total[1]) - jnp.sum(target * shifted, axis=0, keepdims=True)
    score_grad = probability - target
    pre_grad = score_grad * w_score * (sig * (1.0 + pre * (1.0 - sig)))
    pre_grad_bf = pre_grad.astype(BF)
    pre_grad_ref[...] = pre_grad_bf
    dense_ref[...] = lax.dot_general(
        inputs, pre_grad_bf, (((0,), (0,)), ((), ())), preferred_element_type=F32
    )
    bias_grad = jnp.sum(pre_grad, axis=0, keepdims=True)
    score_w_grad = jnp.sum(score_grad * hidden, axis=0, keepdims=True)
    start = pl.multiple_of(core_ref[0] * 256, 256)
    for q in range(4):
        columns = slice(EMB * q, EMB * (q + 1))
        keep_ref[256 * q : 256 * (q + 1)] = dense_ref[pl.ds(start, 256), columns]
        send_ref[256 * q : 256 * (q + 1)] = dense_ref[pl.ds(256 - start, 256), columns]
    def rows_of(line, last):
        parts = [line[:, EMB * q : EMB * (q + 1)] for q in range(4)]
        return jnp.concatenate(parts + [last] + [jnp.zeros((3, EMB), F32)], axis=0)

    first_core = jnp.broadcast_to(core_ref[0], (8, EMB)) == 0
    for_zero = rows_of(bias_grad, jnp.broadcast_to(loss, (1, EMB)))
    for_one = rows_of(score_w_grad, jnp.zeros((1, EMB), F32))
    keep_ref[1024:] = jnp.where(first_core, for_zero, for_one)
    send_ref[1024:] = jnp.where(first_core, for_one, for_zero)


def back_kernel(pre_grad_ref, slot_ref, slot_col_ref, w_ref, out_ref):
    w_bf = w_ref[...].astype(BF)
    grad = jnp.dot(pre_grad_ref[...], w_bf.T, preferred_element_type=F32).astype(BF).astype(F32)
    slots, slot_cols = slot_ref[...], slot_col_ref[...]
    values, hots = [], []
    for t in range(TABLES):
        which = jnp.broadcast_to(slot_cols[:, t : t + 1] >> 9, (IMPS, EMB))
        values.append(fanned(grad[:, t * EMB : (t + 1) * EMB], which).astype(BF))
        slot = slots[t : t + 1]
        hots.append(hot_cols(slot & 127, (slot >> 7) & 3, 4))
    placed = jnp.dot(
        jnp.concatenate(hots, axis=1), jnp.concatenate(values, axis=0), preferred_element_type=F32
    )
    part = OWNERS // FOLD
    for f in range(FOLD):
        out_ref[f * part : (f + 1) * part] = (
            placed[:, f * EMB : (f + 1) * EMB].astype(BF).reshape(part, LINES, EMB)
        )


def pack_kernel(line_ref, keep_ref, came_ref, out_ref, small_ref):
    out_ref[:, :LINES] = line_ref[...]
    for x in range(4):
        for z in range(8):
            for y in range(4):
                k = 256 * (z % 4) + 8 * (2 * (4 * x + y) + z // 4)
                tile = keep_ref[k : k + 8] + came_ref[k : k + 8]
                high = tile.astype(BF).astype(F32)
                out_ref[(x * 8 + z) * 4 + y, LINES:] = jnp.concatenate(
                    [high, tile - high], axis=0
                ).astype(BF)
    small_ref[...] = keep_ref[1024:] + came_ref[1024:]


def open_kernel(got_ref, small_ref, id_ref, line_ref, chunk_ref):
    line_ref[:OWNERS] = got_ref[:, :LINES]
    ids = jnp.transpose(id_ref[...])
    line_ref[OWNERS] = (ids >> 6).astype(F32).astype(BF)
    line_ref[OWNERS + 1] = (ids & 63).astype(F32).astype(BF)
    sums = [jnp.zeros((16, EMB), F32) for _ in range(4)]
    for k in range(OWNERS):
        sums[k % 4] = sums[k % 4] + got_ref[k, LINES:].astype(F32)
    total = (sums[0] + sums[1]) + (sums[2] + sums[3])
    tile = total[:8] + total[8:]
    for k in range(8):
        chunk_ref[k, :8] = tile
        chunk_ref[k, 8:] = small_ref[...]


def column_kernel(got_ref, out_ref):
    small = got_ref[0, 8:]
    for z in range(1, 8):
        small = small + got_ref[z, 8:]
    for p in range(16):
        for z in range(8):
            out_ref[p, 8 * z : 8 * (z + 1)] = got_ref[z, :8]
        out_ref[p, 64:] = small


def place_kernel(
    core_ref, own_ref, other_ref, out_ref, wide_ref, buf_ref, sems
):
    core = core_ref[0]
    lines = OWNERS * LINES
    wide_ref[:lines] = own_ref[:OWNERS].reshape(lines, EMB).astype(F32)
    wide_ref[lines:] = other_ref[:OWNERS].reshape(lines, EMB).astype(F32)
    rows = [
        ref[OWNERS].astype(F32).astype(jnp.int32) * 64 + ref[OWNERS + 1].astype(F32).astype(jnp.int32)
        for ref in (own_ref, other_ref)
    ]
    cols = [jnp.transpose(r) for r in rows]
    part = ROWS // 2 // FOLD
    copies = []
    for t in range(TABLES):
        values, hots = [], []
        for s in range(2):
            for r in range(CAP):
                j = CAP * t + r
                line = wide_ref[pl.ds(s * lines + j, OWNERS, stride=LINES), :]
                which = jnp.broadcast_to(cols[s][:, j : j + 1] >> 9, (OWNERS, EMB)) - FOLD * core
                values.append(fanned(line, which).astype(BF))
                row = rows[s][j : j + 1]
                hots.append(hot_cols(row & 127, (row >> 7) & 3, 4))
        total = jnp.dot(
            jnp.concatenate(hots, axis=1), jnp.concatenate(values, axis=0), preferred_element_type=F32
        )
        for f in range(FOLD):
            x = total[:, f * EMB : (f + 1) * EMB]
            mean = jnp.sum(x * x, axis=1, keepdims=True) * (1.0 / EMB)
            buf_ref[t, part * f : part * (f + 1)] = x * (1.0 / (jnp.sqrt(mean) + 1e-06))
        copy = pltpu.make_async_copy(buf_ref.at[t], out_ref.at[t], sems.at[t])
        copy.start()
        copies.append(copy)
    for copy in copies:
        copy.wait()


def squares_of(ref):
    sums = [jnp.zeros((8, EMB), F32) for _ in range(4)]
    for p in range(16):
        for z in range(8):
            tile = ref[p, 8 * z : 8 * (z + 1)]
            sums[z % 4] = sums[z % 4] + tile * tile
    small = ref[0, 64:]
    for p in range(1, 16):
        small = small + ref[p, 64:]
    return (sums[0] + sums[1]) + (sums[2] + sums[3]), small


def square_kernel(own_ref, main_ref, small_ref):
    main_ref[...], small_ref[...] = squares_of(own_ref)


def final_kernel(
    core_ref, own_ref, other_ref, own_main_ref, own_small_ref, w_ref, b_ref, s_ref, loss_ref
):
    start = core_ref[0] * 256
    other_main, other_small = squares_of(other_ref)
    own_small = own_small_ref[...]
    first_core = jnp.broadcast_to(core_ref[0], (8, EMB)) == 0
    bias = jnp.where(first_core, own_small, other_small)
    score = jnp.where(first_core, other_small, own_small)
    square = jnp.sum(bias[0:4] * bias[0:4] + score[0:4] * score[0:4], axis=0, keepdims=True)
    main = own_main_ref[...] + other_main
    square = jnp.sum(square + jnp.sum(main, axis=0, keepdims=True), axis=1, keepdims=True)
    factor = 1.0 / jnp.sqrt(square * (1.0 / (HID * HID + 2 * HID)) + 1e-06)
    for p in range(16):
        for z in range(8):
            row = 8 * (2 * p + z // 4)
            columns = slice(EMB * (z % 4), EMB * (z % 4 + 1))
            w_ref[pl.ds(pl.multiple_of(start + row, 8), 8), columns] = (
                own_ref[p, 8 * z : 8 * (z + 1)] * factor
            )
            w_ref[pl.ds(pl.multiple_of(256 - start + row, 8), 8), columns] = (
                other_ref[p, 8 * z : 8 * (z + 1)] * factor
            )
    b_ref[...] = bias[0:4] * factor
    s_ref[...] = score[0:4] * factor
    loss_ref[...] = bias[4:5] * (1.0 / 512)


def sds(shape, dtype):
    return jax.ShapeDtypeStruct(shape, dtype)


def call(kernel, mib, outs, ins, scratch=(), out_specs=None, flops=1 << 28):
    return pl.pallas_call(
        kernel,
        out_shape=outs,
        in_specs=ins,
        out_specs=(VMEM,) * len(outs) if out_specs is None else out_specs,
        scratch_shapes=list(scratch),
        cost_estimate=pl.CostEstimate(flops=flops, bytes_accessed=1 << 20, transcendentals=0),
        compiler_params=pltpu.CompilerParams(vmem_limit_bytes=mib << 20),
    )


def exchange(array, axes):
    return lax.all_to_all(array, axes, split_axis=0, concat_axis=0, tiled=True)


def whole_step(
    tables, owner_ids, row_ids, session_of, relevance, logit_bias, w_hidden, bias_hidden, w_score
):
    core = lax.axis_index("dp").astype(jnp.int32).reshape(1)
    swap = [(0, 1), (1, 0)]
    i32 = jnp.int32
    wanted, slots, slot_cols = call(
        slots_kernel, 8,
        (sds((OWNERS, LINES), i32), sds((TABLES, IMPS), i32), sds((IMPS, 2 * TABLES), i32)),
        [SMEM, HBM, HBM],
        [pltpu.VMEM((8, 128), i32), pltpu.VMEM((TABLES, IMPS), i32), pltpu.SemaphoreType.DMA((2,))],
    )(
        core,
        pltpu.with_memory_space_constraint(owner_ids.reshape(8, 128), pltpu.HBM),
        pltpu.with_memory_space_constraint(row_ids.reshape(TABLES, IMPS), pltpu.HBM),
    )
    requested = exchange(wanted, TABLE)
    (served,) = call(
        serve_kernel, 24,
        (sds((OWNERS, LINES, EMB), BF),),
        [VMEM, HBM],
        [
            pltpu.VMEM((OWNERS * LINES, EMB), F32),
            pltpu.VMEM((TABLES, ROWS, EMB), BF),
            pltpu.SemaphoreType.DMA((TABLES,)),
        ],
    )(requested, pltpu.with_memory_space_constraint(tables, pltpu.HBM))
    returned = exchange(served, TABLE)
    half = sds((1024 + SMALL, EMB), F32)
    pre_grad, keep, send = call(
        step_kernel, 24,
        (sds((IMPS, HID), BF), half, half),
        [SMEM] + [VMEM] * 8,
        [pltpu.VMEM((HID, HID), F32)],
    )(
        core, returned, slot_cols, session_of, relevance, logit_bias, w_hidden,
        bias_hidden.reshape(1, HID), w_score.reshape(1, HID),
    )
    came = lax.ppermute(send, "dp", swap)
    (lines,) = call(
        back_kernel, 20, (sds((OWNERS, LINES, EMB), BF),), [VMEM] * 4
    )(pre_grad, slots, slot_cols, w_hidden)
    message, small = call(
        pack_kernel, 12,
        (sds((OWNERS, 2 * LINES, EMB), BF), sds((SMALL, EMB), F32)),
        [VMEM] * 3,
    )(lines, keep, came)
    got = exchange(message, TABLE)
    incoming, chunks = call(
        open_kernel, 12,
        (sds((OWNERS + 2, LINES, EMB), BF), sds((8, 8 + SMALL, EMB), F32)),
        [VMEM] * 3,
    )(got, small, requested)
    other = lax.ppermute(incoming, "dp", swap)
    column = exchange(chunks, "z")
    (emb_step,) = call(
        place_kernel, 28,
        (sds((TABLES, ROWS // 2, EMB), F32),),
        [SMEM] + [VMEM] * 2,
        [
            pltpu.VMEM((2 * OWNERS * LINES, EMB), F32),
            pltpu.VMEM((TABLES, ROWS // 2, EMB), F32),
            pltpu.SemaphoreType.DMA((TABLES,)),
        ],
        out_specs=(ANY,),
    )(core, incoming, other)
    (plane,) = call(column_kernel, 12, (sds((16, 64 + SMALL, EMB), F32),), [VMEM])(column)
    mine = exchange(plane, ("x", "y"))
    theirs = lax.ppermute(mine, "dp", swap)
    tile = sds((8, EMB), F32)
    own_main, own_small = call(square_kernel, 8, (tile, tile), [VMEM])(mine)
    step_hidden, step_bias, step_score, loss = call(
        final_kernel, 12,
        (sds((HID, HID), F32), sds((4, 128), F32), sds((4, 128), F32), sds((1, 128), F32)),
        [SMEM] + [VMEM] * 4,
    )(core, mine, theirs, own_main, own_small)
    return emb_step, step_hidden, step_bias.reshape(HID), step_score.reshape(HID), loss[0, 0]


def solution(mesh):
    split = Mesh(mesh.devices.reshape(4, 8, 4, mesh.shape["dp"]), ALL)
    return jax.shard_map(
        whole_step,
        mesh=split,
        in_specs=(
            P(None, TABLE, None),
            P(ALL, None, None, None),
            P(ALL, None, None),
            P(ALL, None),
            P(ALL, None),
            P(ALL, None),
            P(),
            P(),
            P(),
        ),
        out_specs=(P(None, ALL, None), P(), P(), P(), P()),
        check_vma=False,
    )
```

```python
import jax
import jax.numpy as jnp
from jax import lax
from jax.experimental import pallas as pl
from jax.experimental.pallas import tpu as pltpu
from jax.sharding import Mesh
from jax.sharding import PartitionSpec as P


TABLE = ("x", "z", "y")
ALL = ("x", "z", "y", "dp")
TABLES = 4
CAP = 4
LINES = TABLES * CAP
OWNERS = 128
IMPS = 256
EMB = 128
ROWS = 4096
HID = 512
FOLD = 4
SMALL = 8
VMEM = pl.BlockSpec(memory_space=pltpu.VMEM)
ANY = pl.BlockSpec(memory_space=pl.ANY)
BF = jnp.bfloat16
F32 = jnp.float32


HBM = pl.BlockSpec(memory_space=pltpu.HBM)
SMEM = pl.BlockSpec(memory_space=pltpu.SMEM)


def iota(shape, dim):
    return lax.broadcasted_iota(jnp.int32, shape, dim)


def hot_rows(low, block, blocks):
    n = low.shape[0]
    one = jnp.where(iota((n, 128), 1) == low, 1.0, 0.0).astype(BF)
    which = jnp.broadcast_to(block, (n, 128)).astype(F32).astype(BF)
    zero = jnp.zeros((n, 128), BF)
    return jnp.concatenate([jnp.where(which == BF(c), one, zero) for c in range(blocks)], axis=1)


def hot_cols(low, block, blocks):
    n = low.shape[1]
    one = jnp.where(iota((128, n), 0) == low, 1.0, 0.0).astype(BF)
    which = jnp.broadcast_to(block, (128, n)).astype(F32).astype(BF)
    zero = jnp.zeros((128, n), BF)
    return jnp.concatenate([jnp.where(which == BF(c), one, zero) for c in range(blocks)], axis=0)


def chosen(wide, which):
    kept = wide[:, :EMB]
    for f in range(1, FOLD):
        kept = jnp.where(which == f, wide[:, f * EMB : (f + 1) * EMB], kept)
    return kept


def fanned(piece, which):
    zero = jnp.zeros_like(piece)
    return jnp.concatenate([jnp.where(which == f, piece, zero) for f in range(FOLD)], axis=1)


def slots_kernel(core_ref, own_hbm, row_hbm, want_ref, slot_ref, slot_col_ref, own_ref, row_ref, sems):
    copies = [
        pltpu.make_async_copy(own_hbm, own_ref, sems.at[0]),
        pltpu.make_async_copy(row_hbm, row_ref, sems.at[1]),
    ]
    for copy in copies:
        copy.start()
    for copy in copies:
        copy.wait()
    own = own_ref[...]
    own_rows = [
        jnp.concatenate([own[2 * t : 2 * t + 1], own[2 * t + 1 : 2 * t + 2]], axis=1)
        for t in range(TABLES)
    ]
    own_cols = jnp.transpose(jnp.concatenate(own_rows + own_rows, axis=0))
    row_cols = jnp.transpose(jnp.concatenate([row_ref[...], row_ref[...]], axis=0))
    before = iota((IMPS, IMPS), 0) < iota((IMPS, IMPS), 1)
    slots = []
    for t in range(TABLES):
        same = (own_cols[:, t : t + 1] == own_rows[t]) & before
        rank = jnp.sum(jnp.where(same, 1, 0), axis=0, keepdims=True)
        slots.append(own_rows[t] * LINES + (CAP * t) + rank)
    slot_ref[...] = jnp.concatenate(slots, axis=0)
    slot_cols = jnp.transpose(jnp.concatenate(slots + slots, axis=0))
    slot_col_ref[...] = slot_cols
    lines = []
    for t in range(TABLES):
        slot = jnp.broadcast_to(slot_cols[:, t : t + 1], (IMPS, OWNERS))
        row = jnp.broadcast_to(row_cols[:, t : t + 1], (IMPS, OWNERS))
        for r in range(CAP):
            target = iota((IMPS, OWNERS), 1) * LINES + (CAP * t + r)
            lines.append(jnp.sum(jnp.where(slot == target, row, 0), axis=0, keepdims=True))
    want_ref[...] = jnp.transpose(jnp.concatenate(lines, axis=0))


def serve_kernel(req_ref, far_ref, out_ref, wide_ref, tab_ref, sems):
    copies = [pltpu.make_async_copy(far_ref.at[t], tab_ref.at[t], sems.at[t]) for t in range(TABLES)]
    copies[0].start()
    req = req_ref[...]
    part = ROWS // FOLD
    for t in range(TABLES):
        rows = [req[:, CAP * t + r : CAP * t + r + 1] for r in range(CAP)]
        hot = jnp.concatenate([hot_rows(row & 127, (row >> 7) & 7, 8) for row in rows], axis=0)
        if t + 1 < TABLES:
            copies[t + 1].start()
        copies[t].wait()
        table = jnp.concatenate(
            [tab_ref[t, f * part : (f + 1) * part, :] for f in range(FOLD)], axis=1
        )
        wide = jnp.dot(hot, table, preferred_element_type=F32)
        for r in range(CAP):
            which = jnp.broadcast_to(rows[r] >> 10, (OWNERS, EMB))
            wide_ref[pl.ds(CAP * t + r, OWNERS, stride=LINES), :] = chosen(
                wide[r * OWNERS : (r + 1) * OWNERS], which
            )
    out_ref[...] = wide_ref[...].astype(BF).reshape(OWNERS, LINES, EMB)


def step_kernel(
    core_ref, ret_ref, slot_col_ref, ses_ref, rel_ref, lb_ref, w_ref, b_ref, ws_ref,
    pre_grad_ref, keep_ref, send_ref, dense_ref,
):
    back = ret_ref[...].reshape(OWNERS * LINES, EMB)
    half = OWNERS * LINES // 2
    source = jnp.concatenate([back[:half], back[half:]], axis=1)
    slot_cols = slot_col_ref[...]
    pieces = []
    for t in range(TABLES):
        slot = slot_cols[:, t : t + 1]
        both = jnp.dot(hot_rows(slot & 127, (slot >> 7) & 7, 8), source, preferred_element_type=F32)
        upper = jnp.broadcast_to(slot, (IMPS, EMB)) >= half
        pieces.append(jnp.where(upper, both[:, EMB:], both[:, :EMB]).astype(BF))
    inputs = jnp.concatenate(pieces, axis=1)
    w_bf = w_ref[...].astype(BF)
    w_score = ws_ref[...]
    pre = jnp.dot(inputs, w_bf, preferred_element_type=F32) + b_ref[...]
    sig = jax.nn.sigmoid(pre)
    hidden = pre * sig
    aux = jnp.transpose(
        jnp.concatenate(
            [rel_ref[...], lb_ref[...], ses_ref[...].astype(F32)] + [rel_ref[...]] * 5, axis=0
        )
    )
    relevance, bias_col, session = aux[:, 0:1], aux[:, 1:2], aux[:, 2:3]
    scores = jnp.sum(hidden * w_score, axis=1, keepdims=True) + bias_col
    first = session < 0.5
    low = jnp.float32(-jnp.inf)
    top = [jnp.max(jnp.where(m, scores, low), axis=0, keepdims=True) for m in (first, ~first)]
    shifted = scores - jnp.where(first, top[0], top[1])
    exponent = jnp.exp(shifted)
    total = [jnp.sum(jnp.where(m, exponent, 0.0), axis=0, keepdims=True) for m in (first, ~first)]
    weight = [jnp.sum(jnp.where(m, relevance, 0.0), axis=0, keepdims=True) for m in (first, ~first)]
    probability = exponent / jnp.where(first, total[0], total[1])
    target = relevance / jnp.where(first, weight[0], weight[1])
    loss = jnp.log(total[0]) + jnp.log(total[1]) - jnp.sum(target * shifted, axis=0, keepdims=True)
    score_grad = probability - target
    pre_grad = score_grad * w_score * (sig * (1.0 + pre * (1.0 - sig)))
    pre_grad_bf = pre_grad.astype(BF)
    pre_grad_ref[...] = pre_grad_bf
    dense_ref[...] = lax.dot_general(
        inputs, pre_grad_bf, (((0,), (0,)), ((), ())), preferred_element_type=F32
    )
    bias_grad = jnp.sum(pre_grad, axis=0, keepdims=True)
    score_w_grad = jnp.sum(score_grad * hidden, axis=0, keepdims=True)
    start = pl.multiple_of(core_ref[0] * 256, 256)
    for q in range(4):
        columns = slice(EMB * q, EMB * (q + 1))
        keep_ref[256 * q : 256 * (q + 1)] = dense_ref[pl.ds(start, 256), columns]
        send_ref[256 * q : 256 * (q + 1)] = dense_ref[pl.ds(256 - start, 256), columns]

    def rows_of(line, last):
        parts = [line[:, EMB * q : EMB * (q + 1)] for q in range(4)]
        return jnp.concatenate(parts + [last] + [jnp.zeros((3, EMB), F32)], axis=0)

    first_core = jnp.broadcast_to(core_ref[0], (8, EMB)) == 0
    for_zero = rows_of(bias_grad, jnp.broadcast_to(loss, (1, EMB)))
    for_one = rows_of(score_w_grad, jnp.zeros((1, EMB), F32))
    keep_ref[1024:] = jnp.where(first_core, for_zero, for_one)
    send_ref[1024:] = jnp.where(first_core, for_one, for_zero)


def back_kernel(pre_grad_ref, slot_ref, slot_col_ref, w_ref, out_ref):
    w_bf = w_ref[...].astype(BF)
    grad = jnp.dot(pre_grad_ref[...], w_bf.T, preferred_element_type=F32).astype(BF).astype(F32)
    slots, slot_cols = slot_ref[...], slot_col_ref[...]
    values, hots = [], []
    for t in range(TABLES):
        which = jnp.broadcast_to(slot_cols[:, t : t + 1] >> 9, (IMPS, EMB))
        values.append(fanned(grad[:, t * EMB : (t + 1) * EMB], which).astype(BF))
        slot = slots[t : t + 1]
        hots.append(hot_cols(slot & 127, (slot >> 7) & 3, 4))
    placed = jnp.dot(
        jnp.concatenate(hots, axis=1), jnp.concatenate(values, axis=0), preferred_element_type=F32
    )
    part = OWNERS // FOLD
    for f in range(FOLD):
        out_ref[f * part : (f + 1) * part] = (
            placed[:, f * EMB : (f + 1) * EMB].astype(BF).reshape(part, LINES, EMB)
        )


def pack_kernel(line_ref, keep_ref, came_ref, out_ref, small_ref):
    out_ref[:, :LINES] = line_ref[...]
    for x in range(4):
        for z in range(8):
            for y in range(4):
                k = 256 * (z % 4) + 16 * (4 * x + y) + 4 * (z // 4)
                half = keep_ref[k : k + 4] + came_ref[k : k + 4]
                high = half.astype(BF).astype(F32)
                out_ref[(x * 8 + z) * 4 + y, LINES:] = jnp.concatenate(
                    [high, half - high], axis=0
                ).astype(BF)
    small_ref[...] = keep_ref[1024:] + came_ref[1024:]


def chip_kernel(at_ref, keep_ref, came_ref, own_ref, one_ref, two_ref, three_ref, sum_ref):
    for y in range(4):
        for x in range(4):
            for q in range(4):
                k, to = 256 * q + 16 * (4 * x + y) + 8, 8 * ((y * 4 + x) * 4 + q)
                sum_ref[to : to + 8] = keep_ref[k : k + 8] + came_ref[k : k + 8]
    for d, ref in enumerate((own_ref, one_ref, two_ref, three_ref)):
        ref[...] = sum_ref[pl.ds(pl.multiple_of(((at_ref[0] + d) & 3) * 128, 128), 128), :]


def cross_kernel(
    at_ref, mine_ref, a_ref, b_ref, c_ref, own_ref, one_ref, two_ref, three_ref, sum_ref
):
    sum_ref[...] = (mine_ref[...] + a_ref[...]) + (b_ref[...] + c_ref[...])
    for d, ref in enumerate((own_ref, one_ref, two_ref, three_ref)):
        ref[...] = sum_ref[pl.ds(pl.multiple_of(((at_ref[0] + d) & 3) * 32, 32), 32), :]


def plane_kernel(mine_ref, a_ref, b_ref, c_ref, out_ref):
    out_ref[...] = (mine_ref[...] + a_ref[...]) + (b_ref[...] + c_ref[...])


def open_kernel(got_ref, small_ref, plane_ref, id_ref, line_ref, chunk_ref):
    line_ref[:OWNERS] = got_ref[:, :LINES]
    ids = jnp.transpose(id_ref[...])
    line_ref[OWNERS] = (ids >> 6).astype(F32).astype(BF)
    line_ref[OWNERS + 1] = (ids & 63).astype(F32).astype(BF)
    sums = [jnp.zeros((8, EMB), F32) for _ in range(4)]
    for k in range(OWNERS):
        sums[k % 4] = sums[k % 4] + got_ref[k, LINES:].astype(F32)
    total = (sums[0] + sums[1]) + (sums[2] + sums[3])
    half = total[:4] + total[4:]
    last = jnp.concatenate([half, jnp.zeros((4, EMB), F32)], axis=0)
    for k in range(8):
        chunk_ref[k, :32] = plane_ref[...]
        chunk_ref[k, 32:40] = small_ref[...]
        chunk_ref[k, 40:] = last


def column_kernel(got_ref, out_ref):
    total = got_ref[0, :40]
    for z in range(1, 8):
        total = total + got_ref[z, :40]
    tiles = [
        jnp.concatenate([got_ref[q, 40:44], got_ref[q + 4, 40:44]], axis=0) for q in range(4)
    ]
    column = jnp.concatenate(tiles + [total], axis=0)
    for p in range(16):
        out_ref[p] = column


def place_kernel(
    core_ref, own_ref, other_ref, out_ref, wide_ref, buf_ref, sems
):
    core = core_ref[0]
    lines = OWNERS * LINES
    wide_ref[:lines] = own_ref[:OWNERS].reshape(lines, EMB).astype(F32)
    wide_ref[lines:] = other_ref[:OWNERS].reshape(lines, EMB).astype(F32)
    rows = [
        ref[OWNERS].astype(F32).astype(jnp.int32) * 64 + ref[OWNERS + 1].astype(F32).astype(jnp.int32)
        for ref in (own_ref, other_ref)
    ]
    cols = [jnp.transpose(r) for r in rows]
    part = ROWS // 2 // FOLD
    copies = []
    for t in range(TABLES):
        values, hots = [], []
        for s in range(2):
            for r in range(CAP):
                j = CAP * t + r
                line = wide_ref[pl.ds(s * lines + j, OWNERS, stride=LINES), :]
                which = jnp.broadcast_to(cols[s][:, j : j + 1] >> 9, (OWNERS, EMB)) - FOLD * core
                values.append(fanned(line, which).astype(BF))
                row = rows[s][j : j + 1]
                hots.append(hot_cols(row & 127, (row >> 7) & 3, 4))
        total = jnp.dot(
            jnp.concatenate(hots, axis=1), jnp.concatenate(values, axis=0), preferred_element_type=F32
        )
        for f in range(FOLD):
            x = total[:, f * EMB : (f + 1) * EMB]
            mean = jnp.sum(x * x, axis=1, keepdims=True) * (1.0 / EMB)
            buf_ref[t, part * f : part * (f + 1)] = x * (1.0 / (jnp.sqrt(mean) + 1e-06))
        copy = pltpu.make_async_copy(buf_ref.at[t], out_ref.at[t], sems.at[t])
        copy.start()
        copies.append(copy)
    for copy in copies:
        copy.wait()


def squares_of(ref):
    sums = [jnp.zeros((8, EMB), F32) for _ in range(4)]
    for p in range(16):
        for z in range(8):
            tile = ref[p, 8 * z : 8 * (z + 1)]
            sums[z % 4] = sums[z % 4] + tile * tile
    small = ref[0, 64:]
    for p in range(1, 16):
        small = small + ref[p, 64:]
    return (sums[0] + sums[1]) + (sums[2] + sums[3]), small


def square_kernel(own_ref, main_ref, small_ref):
    main_ref[...], small_ref[...] = squares_of(own_ref)


def final_kernel(
    core_ref, own_ref, other_ref, own_main_ref, own_small_ref, w_ref, b_ref, s_ref, loss_ref
):
    start = core_ref[0] * 256
    other_main, other_small = squares_of(other_ref)
    own_small = own_small_ref[...]
    first_core = jnp.broadcast_to(core_ref[0], (8, EMB)) == 0
    bias = jnp.where(first_core, own_small, other_small)
    score = jnp.where(first_core, other_small, own_small)
    square = jnp.sum(bias[0:4] * bias[0:4] + score[0:4] * score[0:4], axis=0, keepdims=True)
    main = own_main_ref[...] + other_main
    square = jnp.sum(square + jnp.sum(main, axis=0, keepdims=True), axis=1, keepdims=True)
    factor = 1.0 / jnp.sqrt(square * (1.0 / (HID * HID + 2 * HID)) + 1e-06)
    for p in range(16):
        for z in range(8):
            row = 8 * (2 * p + z // 4)
            columns = slice(EMB * (z % 4), EMB * (z % 4 + 1))
            w_ref[pl.ds(pl.multiple_of(start + row, 8), 8), columns] = (
                own_ref[p, 8 * z : 8 * (z + 1)] * factor
            )
            w_ref[pl.ds(pl.multiple_of(256 - start + row, 8), 8), columns] = (
                other_ref[p, 8 * z : 8 * (z + 1)] * factor
            )
    b_ref[...] = bias[0:4] * factor
    s_ref[...] = score[0:4] * factor
    loss_ref[...] = bias[4:5] * (1.0 / 512)


def sds(shape, dtype):
    return jax.ShapeDtypeStruct(shape, dtype)


def call(kernel, mib, outs, ins, scratch=(), out_specs=None, flops=1 << 28):
    return pl.pallas_call(
        kernel,
        out_shape=outs,
        in_specs=ins,
        out_specs=(VMEM,) * len(outs) if out_specs is None else out_specs,
        scratch_shapes=list(scratch),
        cost_estimate=pl.CostEstimate(flops=flops, bytes_accessed=1 << 20, transcendentals=0),
        compiler_params=pltpu.CompilerParams(vmem_limit_bytes=mib << 20),
    )


def exchange(array, axes):
    return lax.all_to_all(array, axes, split_axis=0, concat_axis=0, tiled=True)


def whole_step(
    tables, owner_ids, row_ids, session_of, relevance, logit_bias, w_hidden, bias_hidden, w_score
):
    core = lax.axis_index("dp").astype(jnp.int32).reshape(1)
    swap = [(0, 1), (1, 0)]
    i32 = jnp.int32
    wanted, slots, slot_cols = call(
        slots_kernel, 8,
        (sds((OWNERS, LINES), i32), sds((TABLES, IMPS), i32), sds((IMPS, 2 * TABLES), i32)),
        [SMEM, HBM, HBM],
        [pltpu.VMEM((8, 128), i32), pltpu.VMEM((TABLES, IMPS), i32), pltpu.SemaphoreType.DMA((2,))],
    )(
        core,
        pltpu.with_memory_space_constraint(owner_ids.reshape(8, 128), pltpu.HBM),
        pltpu.with_memory_space_constraint(row_ids.reshape(TABLES, IMPS), pltpu.HBM),
    )
    requested = exchange(wanted, TABLE)
    (served,) = call(
        serve_kernel, 24,
        (sds((OWNERS, LINES, EMB), BF),),
        [VMEM, HBM],
        [
            pltpu.VMEM((OWNERS * LINES, EMB), F32),
            pltpu.VMEM((TABLES, ROWS, EMB), BF),
            pltpu.SemaphoreType.DMA((TABLES,)),
        ],
    )(requested, pltpu.with_memory_space_constraint(tables, pltpu.HBM))
    returned = exchange(served, TABLE)
    half = sds((1024 + SMALL, EMB), F32)
    pre_grad, keep, send = call(
        step_kernel, 24,
        (sds((IMPS, HID), BF), half, half),
        [SMEM] + [VMEM] * 8,
        [pltpu.VMEM((HID, HID), F32)],
    )(
        core, returned, slot_cols, session_of, relevance, logit_bias, w_hidden,
        bias_hidden.reshape(1, HID), w_score.reshape(1, HID),
    )
    came = lax.ppermute(send, "dp", swap)
    (lines,) = call(
        back_kernel, 20, (sds((OWNERS, LINES, EMB), BF),), [VMEM] * 4
    )(pre_grad, slots, slot_cols, w_hidden)
    message, small = call(
        pack_kernel, 12,
        (sds((OWNERS, LINES + 8, EMB), BF), sds((SMALL, EMB), F32)),
        [VMEM] * 3,
    )(lines, keep, came)
    got = exchange(message, TABLE)

    def spread(parts, axis):
        return [
            lax.ppermute(part, axis, [(i, (i + d) % 4) for i in range(4)])
            for d, part in enumerate(parts, 1)
        ]

    quarter, tiles = sds((128, EMB), F32), sds((32, EMB), F32)
    own, *rest = call(
        chip_kernel, 8, (quarter,) * 4, [SMEM] + [VMEM] * 2,
        [pltpu.VMEM((512, EMB), F32)],
    )(lax.axis_index("y").astype(i32).reshape(1), keep, came)
    rest = spread(rest, "y")
    own, *rest = call(
        cross_kernel, 8, (tiles,) * 4, [SMEM] + [VMEM] * 4,
        [pltpu.VMEM((128, EMB), F32)],
    )(lax.axis_index("x").astype(i32).reshape(1), own, *rest)
    rest = spread(rest, "x")
    (plane,) = call(plane_kernel, 8, (tiles,), [VMEM] * 4)(own, *rest)
    incoming, chunks = call(
        open_kernel, 12,
        (sds((OWNERS + 2, LINES, EMB), BF), sds((8, 48, EMB), F32)),
        [VMEM] * 4,
    )(got, small, plane, requested)
    other = lax.ppermute(incoming, "dp", swap)
    column = exchange(chunks, "z")
    (emb_step,) = call(
        place_kernel, 28,
        (sds((TABLES, ROWS // 2, EMB), F32),),
        [SMEM] + [VMEM] * 2,
        [
            pltpu.VMEM((2 * OWNERS * LINES, EMB), F32),
            pltpu.VMEM((TABLES, ROWS // 2, EMB), F32),
            pltpu.SemaphoreType.DMA((TABLES,)),
        ],
        out_specs=(ANY,),
    )(core, incoming, other)
    (sums,) = call(column_kernel, 12, (sds((16, 64 + SMALL, EMB), F32),), [VMEM])(column)
    mine = exchange(sums, ("x", "y"))
    theirs = lax.ppermute(mine, "dp", swap)
    tile = sds((8, EMB), F32)
    own_main, own_small = call(square_kernel, 8, (tile, tile), [VMEM])(mine)
    step_hidden, step_bias, step_score, loss = call(
        final_kernel, 12,
        (sds((HID, HID), F32), sds((4, 128), F32), sds((4, 128), F32), sds((1, 128), F32)),
        [SMEM] + [VMEM] * 4,
    )(core, mine, theirs, own_main, own_small)
    return emb_step, step_hidden, step_bias.reshape(HID), step_score.reshape(HID), loss[0, 0]


def solution(mesh):
    split = Mesh(mesh.devices.reshape(4, 8, 4, mesh.shape["dp"]), ALL)
    return jax.shard_map(
        whole_step,
        mesh=split,
        in_specs=(
            P(None, TABLE, None),
            P(ALL, None, None, None),
            P(ALL, None, None),
            P(ALL, None),
            P(ALL, None),
            P(ALL, None),
            P(),
            P(),
            P(),
        ),
        out_specs=(P(None, ALL, None), P(), P(), P(), P()),
        check_vma=False,
    )
```

```python
import jax
import jax.numpy as jnp
from jax import lax
from jax.experimental import pallas as pl
from jax.experimental.pallas import tpu as pltpu
from jax.sharding import Mesh
from jax.sharding import PartitionSpec as P


TABLE = ("x", "z", "y")
ALL = ("x", "z", "y", "dp")
TABLES = 4
CAP = 4
LINES = TABLES * CAP
OWNERS = 128
IMPS = 256
EMB = 128
ROWS = 4096
HID = 512
FOLD = 4
SMALL = 8
VMEM = pl.BlockSpec(memory_space=pltpu.VMEM)
ANY = pl.BlockSpec(memory_space=pl.ANY)
BF = jnp.bfloat16
F32 = jnp.float32


HBM = pl.BlockSpec(memory_space=pltpu.HBM)
SMEM = pl.BlockSpec(memory_space=pltpu.SMEM)


def iota(shape, dim):
    return lax.broadcasted_iota(jnp.int32, shape, dim)


def hot_rows(low, block, blocks):
    n = low.shape[0]
    one = jnp.where(iota((n, 128), 1) == low, 1.0, 0.0).astype(BF)
    which = jnp.broadcast_to(block, (n, 128)).astype(F32).astype(BF)
    zero = jnp.zeros((n, 128), BF)
    return jnp.concatenate([jnp.where(which == BF(c), one, zero) for c in range(blocks)], axis=1)


def hot_cols(low, block, blocks):
    n = low.shape[1]
    one = jnp.where(iota((128, n), 0) == low, 1.0, 0.0).astype(BF)
    which = jnp.broadcast_to(block, (128, n)).astype(F32).astype(BF)
    zero = jnp.zeros((128, n), BF)
    return jnp.concatenate([jnp.where(which == BF(c), one, zero) for c in range(blocks)], axis=0)


def chosen(wide, which):
    kept = wide[:, :EMB]
    for f in range(1, FOLD):
        kept = jnp.where(which == f, wide[:, f * EMB : (f + 1) * EMB], kept)
    return kept


def fanned(piece, which):
    zero = jnp.zeros_like(piece)
    return jnp.concatenate([jnp.where(which == f, piece, zero) for f in range(FOLD)], axis=1)


def slots_kernel(core_ref, own_hbm, row_hbm, want_ref, slot_ref, slot_col_ref, own_ref, row_ref, sems):
    copies = [
        pltpu.make_async_copy(own_hbm, own_ref, sems.at[0]),
        pltpu.make_async_copy(row_hbm, row_ref, sems.at[1]),
    ]
    for copy in copies:
        copy.start()
    for copy in copies:
        copy.wait()
    own = own_ref[...]
    own_rows = [
        jnp.concatenate([own[2 * t : 2 * t + 1], own[2 * t + 1 : 2 * t + 2]], axis=1)
        for t in range(TABLES)
    ]
    own_cols = jnp.transpose(jnp.concatenate(own_rows + own_rows, axis=0))
    row_cols = jnp.transpose(jnp.concatenate([row_ref[...], row_ref[...]], axis=0))
    before = iota((IMPS, IMPS), 0) < iota((IMPS, IMPS), 1)
    slots = []
    for t in range(TABLES):
        same = (own_cols[:, t : t + 1] == own_rows[t]) & before
        rank = jnp.sum(jnp.where(same, 1, 0), axis=0, keepdims=True)
        slots.append(own_rows[t] * LINES + (CAP * t) + rank)
    slot_ref[...] = jnp.concatenate(slots, axis=0)
    slot_cols = jnp.transpose(jnp.concatenate(slots + slots, axis=0))
    slot_col_ref[...] = slot_cols
    lines = []
    for t in range(TABLES):
        slot = jnp.broadcast_to(slot_cols[:, t : t + 1], (IMPS, OWNERS))
        row = jnp.broadcast_to(row_cols[:, t : t + 1], (IMPS, OWNERS))
        for r in range(CAP):
            target = iota((IMPS, OWNERS), 1) * LINES + (CAP * t + r)
            lines.append(jnp.sum(jnp.where(slot == target, row, 0), axis=0, keepdims=True))
    want_ref[...] = jnp.transpose(jnp.concatenate(lines, axis=0))


def serve_kernel(req_ref, far_ref, out_ref, wide_ref, tab_ref, sems):
    copies = [pltpu.make_async_copy(far_ref.at[t], tab_ref.at[t], sems.at[t]) for t in range(TABLES)]
    for copy in copies:
        copy.start()
    req = req_ref[...]
    part = ROWS // FOLD
    for t in range(TABLES):
        rows = [req[:, CAP * t + r : CAP * t + r + 1] for r in range(CAP)]
        hot = jnp.concatenate([hot_rows(row & 127, (row >> 7) & 7, 8) for row in rows], axis=0)
        copies[t].wait()
        table = jnp.concatenate(
            [tab_ref[t, f * part : (f + 1) * part, :] for f in range(FOLD)], axis=1
        )
        wide = jnp.dot(hot, table, preferred_element_type=F32)
        for r in range(CAP):
            which = jnp.broadcast_to(rows[r] >> 10, (OWNERS, EMB))
            wide_ref[pl.ds(CAP * t + r, OWNERS, stride=LINES), :] = chosen(
                wide[r * OWNERS : (r + 1) * OWNERS], which
            )
    out_ref[...] = wide_ref[...].astype(BF).reshape(OWNERS, LINES, EMB)


def step_kernel(
    core_ref, ret_ref, slot_col_ref, ses_ref, rel_ref, lb_ref, w_ref, b_ref, ws_ref,
    pre_grad_ref, keep_ref, send_ref, dense_ref,
):
    back = ret_ref[...].reshape(OWNERS * LINES, EMB)
    half = OWNERS * LINES // 2
    source = jnp.concatenate([back[:half], back[half:]], axis=1)
    slot_cols = slot_col_ref[...]
    pieces = []
    for t in range(TABLES):
        slot = slot_cols[:, t : t + 1]
        both = jnp.dot(hot_rows(slot & 127, (slot >> 7) & 7, 8), source, preferred_element_type=F32)
        upper = jnp.broadcast_to(slot, (IMPS, EMB)) >= half
        pieces.append(jnp.where(upper, both[:, EMB:], both[:, :EMB]).astype(BF))
    inputs = jnp.concatenate(pieces, axis=1)
    w_bf = w_ref[...].astype(BF)
    w_score = ws_ref[...]
    pre = jnp.dot(inputs, w_bf, preferred_element_type=F32) + b_ref[...]
    sig = jax.nn.sigmoid(pre)
    hidden = pre * sig
    aux = jnp.transpose(
        jnp.concatenate(
            [rel_ref[...], lb_ref[...], ses_ref[...].astype(F32)] + [rel_ref[...]] * 5, axis=0
        )
    )
    relevance, bias_col, session = aux[:, 0:1], aux[:, 1:2], aux[:, 2:3]
    scores = jnp.sum(hidden * w_score, axis=1, keepdims=True) + bias_col
    first = session < 0.5
    low = jnp.float32(-jnp.inf)
    top = [jnp.max(jnp.where(m, scores, low), axis=0, keepdims=True) for m in (first, ~first)]
    shifted = scores - jnp.where(first, top[0], top[1])
    exponent = jnp.exp(shifted)
    total = [jnp.sum(jnp.where(m, exponent, 0.0), axis=0, keepdims=True) for m in (first, ~first)]
    weight = [jnp.sum(jnp.where(m, relevance, 0.0), axis=0, keepdims=True) for m in (first, ~first)]
    probability = exponent / jnp.where(first, total[0], total[1])
    target = relevance / jnp.where(first, weight[0], weight[1])
    loss = jnp.log(total[0]) + jnp.log(total[1]) - jnp.sum(target * shifted, axis=0, keepdims=True)
    score_grad = probability - target
    pre_grad = score_grad * w_score * (sig * (1.0 + pre * (1.0 - sig)))
    pre_grad_bf = pre_grad.astype(BF)
    pre_grad_ref[...] = pre_grad_bf
    dense_ref[...] = lax.dot_general(
        inputs, pre_grad_bf, (((0,), (0,)), ((), ())), preferred_element_type=F32
    )
    bias_grad = jnp.sum(pre_grad, axis=0, keepdims=True)
    score_w_grad = jnp.sum(score_grad * hidden, axis=0, keepdims=True)
    start = pl.multiple_of(core_ref[0] * 256, 256)
    for q in range(4):
        columns = slice(EMB * q, EMB * (q + 1))
        keep_ref[256 * q : 256 * (q + 1)] = dense_ref[pl.ds(start, 256), columns]
        send_ref[256 * q : 256 * (q + 1)] = dense_ref[pl.ds(256 - start, 256), columns]

    def rows_of(line, last):
        parts = [line[:, EMB * q : EMB * (q + 1)] for q in range(4)]
        return jnp.concatenate(parts + [last] + [jnp.zeros((3, EMB), F32)], axis=0)

    first_core = jnp.broadcast_to(core_ref[0], (8, EMB)) == 0
    for_zero = rows_of(bias_grad, jnp.broadcast_to(loss, (1, EMB)))
    for_one = rows_of(score_w_grad, jnp.zeros((1, EMB), F32))
    keep_ref[1024:] = jnp.where(first_core, for_zero, for_one)
    send_ref[1024:] = jnp.where(first_core, for_one, for_zero)


def back_kernel(pre_grad_ref, slot_ref, slot_col_ref, w_ref, out_ref):
    w_bf = w_ref[...].astype(BF)
    grad = jnp.dot(pre_grad_ref[...], w_bf.T, preferred_element_type=F32).astype(BF).astype(F32)
    slots, slot_cols = slot_ref[...], slot_col_ref[...]
    values, hots = [], []
    for t in range(TABLES):
        which = jnp.broadcast_to(slot_cols[:, t : t + 1] >> 9, (IMPS, EMB))
        values.append(fanned(grad[:, t * EMB : (t + 1) * EMB], which).astype(BF))
        slot = slots[t : t + 1]
        hots.append(hot_cols(slot & 127, (slot >> 7) & 3, 4))
    placed = jnp.dot(
        jnp.concatenate(hots, axis=1), jnp.concatenate(values, axis=0), preferred_element_type=F32
    )
    part = OWNERS // FOLD
    for f in range(FOLD):
        out_ref[f * part : (f + 1) * part] = (
            placed[:, f * EMB : (f + 1) * EMB].astype(BF).reshape(part, LINES, EMB)
        )


def pack_kernel(line_ref, keep_ref, came_ref, out_ref, small_ref):
    out_ref[:, :LINES] = line_ref[...]
    for x in range(4):
        for z in range(8):
            for y in range(4):
                k = 256 * (z % 4) + 16 * (4 * x + y) + 4 * (z // 4)
                half = keep_ref[k : k + 4] + came_ref[k : k + 4]
                high = half.astype(BF).astype(F32)
                out_ref[(x * 8 + z) * 4 + y, LINES:] = jnp.concatenate(
                    [high, half - high], axis=0
                ).astype(BF)
    small_ref[...] = keep_ref[1024:] + came_ref[1024:]


def chip_kernel(at_ref, keep_ref, came_ref, own_ref, one_ref, two_ref, three_ref, sum_ref):
    for y in range(4):
        for x in range(4):
            for q in range(4):
                k, to = 256 * q + 16 * (4 * x + y) + 8, 8 * ((y * 4 + x) * 4 + q)
                sum_ref[to : to + 8] = keep_ref[k : k + 8] + came_ref[k : k + 8]
    for d, ref in enumerate((own_ref, one_ref, two_ref, three_ref)):
        ref[...] = sum_ref[pl.ds(pl.multiple_of(((at_ref[0] + d) & 3) * 128, 128), 128), :]


def cross_kernel(
    at_ref, mine_ref, a_ref, b_ref, c_ref, own_ref, one_ref, two_ref, three_ref, sum_ref
):
    sum_ref[...] = (mine_ref[...] + a_ref[...]) + (b_ref[...] + c_ref[...])
    for d, ref in enumerate((own_ref, one_ref, two_ref, three_ref)):
        ref[...] = sum_ref[pl.ds(pl.multiple_of(((at_ref[0] + d) & 3) * 32, 32), 32), :]


def plane_kernel(mine_ref, a_ref, b_ref, c_ref, out_ref):
    out_ref[...] = (mine_ref[...] + a_ref[...]) + (b_ref[...] + c_ref[...])


def lines_kernel(got_ref, id_ref, line_ref):
    line_ref[:OWNERS] = got_ref[:, :LINES]
    ids = jnp.transpose(id_ref[...])
    line_ref[OWNERS] = (ids >> 6).astype(F32).astype(BF)
    line_ref[OWNERS + 1] = (ids & 63).astype(F32).astype(BF)


def open_kernel(got_ref, small_ref, plane_ref, chunk_ref):
    sums = [jnp.zeros((8, EMB), F32) for _ in range(4)]
    for k in range(OWNERS):
        sums[k % 4] = sums[k % 4] + got_ref[k, LINES:].astype(F32)
    total = (sums[0] + sums[1]) + (sums[2] + sums[3])
    half = total[:4] + total[4:]
    last = jnp.concatenate([half, jnp.zeros((4, EMB), F32)], axis=0)
    for k in range(8):
        chunk_ref[k, :32] = plane_ref[...]
        chunk_ref[k, 32:40] = small_ref[...]
        chunk_ref[k, 40:] = last


def column_kernel(got_ref, out_ref):
    total = got_ref[0, :40]
    for z in range(1, 8):
        total = total + got_ref[z, :40]
    tiles = [
        jnp.concatenate([got_ref[q, 40:44], got_ref[q + 4, 40:44]], axis=0) for q in range(4)
    ]
    column = jnp.concatenate(tiles + [total], axis=0)
    for p in range(16):
        out_ref[p] = column


def place_kernel(
    core_ref, own_ref, other_ref, out_ref, wide_ref, buf_ref, sems
):
    core = core_ref[0]
    lines = OWNERS * LINES
    wide_ref[:lines] = own_ref[:OWNERS].reshape(lines, EMB).astype(F32)
    wide_ref[lines:] = other_ref[:OWNERS].reshape(lines, EMB).astype(F32)
    rows = [
        ref[OWNERS].astype(F32).astype(jnp.int32) * 64 + ref[OWNERS + 1].astype(F32).astype(jnp.int32)
        for ref in (own_ref, other_ref)
    ]
    cols = [jnp.transpose(r) for r in rows]
    part = ROWS // 2 // FOLD
    copies = []
    for t in range(TABLES):
        values, hots = [], []
        for s in range(2):
            for r in range(CAP):
                j = CAP * t + r
                line = wide_ref[pl.ds(s * lines + j, OWNERS, stride=LINES), :]
                which = jnp.broadcast_to(cols[s][:, j : j + 1] >> 9, (OWNERS, EMB)) - FOLD * core
                values.append(fanned(line, which).astype(BF))
                row = rows[s][j : j + 1]
                hots.append(hot_cols(row & 127, (row >> 7) & 3, 4))
        total = jnp.dot(
            jnp.concatenate(hots, axis=1), jnp.concatenate(values, axis=0), preferred_element_type=F32
        )
        for f in range(FOLD):
            x = total[:, f * EMB : (f + 1) * EMB]
            mean = jnp.sum(x * x, axis=1, keepdims=True) * (1.0 / EMB)
            buf_ref[t, part * f : part * (f + 1)] = x * (1.0 / (jnp.sqrt(mean) + 1e-06))
        copy = pltpu.make_async_copy(buf_ref.at[t], out_ref.at[t], sems.at[t])
        copy.start()
        copies.append(copy)
    for copy in copies:
        copy.wait()


def squares_of(ref):
    sums = [jnp.zeros((8, EMB), F32) for _ in range(4)]
    for p in range(16):
        for z in range(8):
            tile = ref[p, 8 * z : 8 * (z + 1)]
            sums[z % 4] = sums[z % 4] + tile * tile
    small = ref[0, 64:]
    for p in range(1, 16):
        small = small + ref[p, 64:]
    return (sums[0] + sums[1]) + (sums[2] + sums[3]), small


def square_kernel(own_ref, main_ref, small_ref):
    main_ref[...], small_ref[...] = squares_of(own_ref)


def final_kernel(
    core_ref, own_ref, other_ref, own_main_ref, own_small_ref, w_ref, b_ref, s_ref, loss_ref
):
    start = core_ref[0] * 256
    other_main, other_small = squares_of(other_ref)
    own_small = own_small_ref[...]
    first_core = jnp.broadcast_to(core_ref[0], (8, EMB)) == 0
    bias = jnp.where(first_core, own_small, other_small)
    score = jnp.where(first_core, other_small, own_small)
    square = jnp.sum(bias[0:4] * bias[0:4] + score[0:4] * score[0:4], axis=0, keepdims=True)
    main = own_main_ref[...] + other_main
    square = jnp.sum(square + jnp.sum(main, axis=0, keepdims=True), axis=1, keepdims=True)
    factor = 1.0 / jnp.sqrt(square * (1.0 / (HID * HID + 2 * HID)) + 1e-06)
    for p in range(16):
        for z in range(8):
            row = 8 * (2 * p + z // 4)
            columns = slice(EMB * (z % 4), EMB * (z % 4 + 1))
            w_ref[pl.ds(pl.multiple_of(start + row, 8), 8), columns] = (
                own_ref[p, 8 * z : 8 * (z + 1)] * factor
            )
            w_ref[pl.ds(pl.multiple_of(256 - start + row, 8), 8), columns] = (
                other_ref[p, 8 * z : 8 * (z + 1)] * factor
            )
    b_ref[...] = bias[0:4] * factor
    s_ref[...] = score[0:4] * factor
    loss_ref[...] = bias[4:5] * (1.0 / 512)


def sds(shape, dtype):
    return jax.ShapeDtypeStruct(shape, dtype)


def call(kernel, mib, outs, ins, scratch=(), out_specs=None, flops=1 << 28):
    return pl.pallas_call(
        kernel,
        out_shape=outs,
        in_specs=ins,
        out_specs=(VMEM,) * len(outs) if out_specs is None else out_specs,
        scratch_shapes=list(scratch),
        cost_estimate=pl.CostEstimate(flops=flops, bytes_accessed=1 << 20, transcendentals=0),
        compiler_params=pltpu.CompilerParams(vmem_limit_bytes=mib << 20),
    )


def exchange(array, axes):
    return lax.all_to_all(array, axes, split_axis=0, concat_axis=0, tiled=True)


def whole_step(
    tables, owner_ids, row_ids, session_of, relevance, logit_bias, w_hidden, bias_hidden, w_score
):
    core = lax.axis_index("dp").astype(jnp.int32).reshape(1)
    swap = [(0, 1), (1, 0)]
    i32 = jnp.int32
    wanted, slots, slot_cols = call(
        slots_kernel, 8,
        (sds((OWNERS, LINES), i32), sds((TABLES, IMPS), i32), sds((IMPS, 2 * TABLES), i32)),
        [SMEM, HBM, HBM],
        [pltpu.VMEM((8, 128), i32), pltpu.VMEM((TABLES, IMPS), i32), pltpu.SemaphoreType.DMA((2,))],
    )(
        core,
        pltpu.with_memory_space_constraint(owner_ids.reshape(8, 128), pltpu.HBM),
        pltpu.with_memory_space_constraint(row_ids.reshape(TABLES, IMPS), pltpu.HBM),
    )
    requested = exchange(wanted, TABLE)
    (served,) = call(
        serve_kernel, 24,
        (sds((OWNERS, LINES, EMB), BF),),
        [VMEM, HBM],
        [
            pltpu.VMEM((OWNERS * LINES, EMB), F32),
            pltpu.VMEM((TABLES, ROWS, EMB), BF),
            pltpu.SemaphoreType.DMA((TABLES,)),
        ],
    )(requested, pltpu.with_memory_space_constraint(tables, pltpu.HBM))
    returned = exchange(served, TABLE)
    half = sds((1024 + SMALL, EMB), F32)
    pre_grad, keep, send = call(
        step_kernel, 24,
        (sds((IMPS, HID), BF), half, half),
        [SMEM] + [VMEM] * 8,
        [pltpu.VMEM((HID, HID), F32)],
    )(
        core, returned, slot_cols, session_of, relevance, logit_bias, w_hidden,
        bias_hidden.reshape(1, HID), w_score.reshape(1, HID),
    )
    came = lax.ppermute(send, "dp", swap)
    (lines,) = call(
        back_kernel, 20, (sds((OWNERS, LINES, EMB), BF),), [VMEM] * 4
    )(pre_grad, slots, slot_cols, w_hidden)
    message, small = call(
        pack_kernel, 12,
        (sds((OWNERS, LINES + 8, EMB), BF), sds((SMALL, EMB), F32)),
        [VMEM] * 3,
    )(lines, keep, came)
    got = exchange(message, TABLE)

    def spread(parts, axis):
        return [
            lax.ppermute(part, axis, [(i, (i + d) % 4) for i in range(4)])
            for d, part in enumerate(parts, 1)
        ]

    quarter, tiles = sds((128, EMB), F32), sds((32, EMB), F32)
    own, *rest = call(
        chip_kernel, 8, (quarter,) * 4, [SMEM] + [VMEM] * 2,
        [pltpu.VMEM((512, EMB), F32)],
    )(lax.axis_index("y").astype(i32).reshape(1), keep, came)
    rest = spread(rest, "y")
    own, *rest = call(
        cross_kernel, 8, (tiles,) * 4, [SMEM] + [VMEM] * 4,
        [pltpu.VMEM((128, EMB), F32)],
    )(lax.axis_index("x").astype(i32).reshape(1), own, *rest)
    rest = spread(rest, "x")
    (plane,) = call(plane_kernel, 8, (tiles,), [VMEM] * 4)(own, *rest)
    (chunks,) = call(open_kernel, 12, (sds((8, 48, EMB), F32),), [VMEM] * 3)(got, small, plane)
    (incoming,) = call(
        lines_kernel, 12, (sds((OWNERS + 2, LINES, EMB), BF),), [VMEM] * 2
    )(got, requested)
    other = lax.ppermute(incoming, "dp", swap)
    column = exchange(chunks, "z")
    (emb_step,) = call(
        place_kernel, 28,
        (sds((TABLES, ROWS // 2, EMB), F32),),
        [SMEM] + [VMEM] * 2,
        [
            pltpu.VMEM((2 * OWNERS * LINES, EMB), F32),
            pltpu.VMEM((TABLES, ROWS // 2, EMB), F32),
            pltpu.SemaphoreType.DMA((TABLES,)),
        ],
        out_specs=(ANY,),
    )(core, incoming, other)
    (sums,) = call(column_kernel, 12, (sds((16, 64 + SMALL, EMB), F32),), [VMEM])(column)
    mine = exchange(sums, ("x", "y"))
    theirs = lax.ppermute(mine, "dp", swap)
    tile = sds((8, EMB), F32)
    own_main, own_small = call(square_kernel, 8, (tile, tile), [VMEM])(mine)
    step_hidden, step_bias, step_score, loss = call(
        final_kernel, 12,
        (sds((HID, HID), F32), sds((4, 128), F32), sds((4, 128), F32), sds((1, 128), F32)),
        [SMEM] + [VMEM] * 4,
    )(core, mine, theirs, own_main, own_small)
    return emb_step, step_hidden, step_bias.reshape(HID), step_score.reshape(HID), loss[0, 0]


def solution(mesh):
    split = Mesh(mesh.devices.reshape(4, 8, 4, mesh.shape["dp"]), ALL)
    return jax.shard_map(
        whole_step,
        mesh=split,
        in_specs=(
            P(None, TABLE, None),
            P(ALL, None, None, None),
            P(ALL, None, None),
            P(ALL, None),
            P(ALL, None),
            P(ALL, None),
            P(),
            P(),
            P(),
        ),
        out_specs=(P(None, ALL, None), P(), P(), P(), P()),
        check_vma=False,
    )
```

```python
import jax
import jax.numpy as jnp
from jax import lax
from jax.experimental import pallas as pl
from jax.experimental.pallas import tpu as pltpu
from jax.sharding import Mesh
from jax.sharding import PartitionSpec as P


TABLE = ("x", "z", "y")
ALL = ("x", "z", "y", "dp")
TABLES = 4
CAP = 4
LINES = TABLES * CAP
OWNERS = 128
IMPS = 256
EMB = 128
ROWS = 4096
HID = 512
FOLD = 4
SMALL = 8
VMEM = pl.BlockSpec(memory_space=pltpu.VMEM)
ANY = pl.BlockSpec(memory_space=pl.ANY)
BF = jnp.bfloat16
F32 = jnp.float32


HBM = pl.BlockSpec(memory_space=pltpu.HBM)
SMEM = pl.BlockSpec(memory_space=pltpu.SMEM)


def iota(shape, dim):
    return lax.broadcasted_iota(jnp.int32, shape, dim)


def hot_rows(low, block, blocks):
    n = low.shape[0]
    one = jnp.where(iota((n, 128), 1) == low, 1.0, 0.0).astype(BF)
    which = jnp.broadcast_to(block, (n, 128)).astype(F32).astype(BF)
    zero = jnp.zeros((n, 128), BF)
    return jnp.concatenate([jnp.where(which == BF(c), one, zero) for c in range(blocks)], axis=1)


def hot_cols(low, block, blocks):
    n = low.shape[1]
    one = jnp.where(iota((128, n), 0) == low, 1.0, 0.0).astype(BF)
    which = jnp.broadcast_to(block, (128, n)).astype(F32).astype(BF)
    zero = jnp.zeros((128, n), BF)
    return jnp.concatenate([jnp.where(which == BF(c), one, zero) for c in range(blocks)], axis=0)


def chosen(wide, which):
    kept = wide[:, :EMB]
    for f in range(1, FOLD):
        kept = jnp.where(which == f, wide[:, f * EMB : (f + 1) * EMB], kept)
    return kept


def fanned(piece, which):
    zero = jnp.zeros_like(piece)
    return jnp.concatenate([jnp.where(which == f, piece, zero) for f in range(FOLD)], axis=1)


def slots_kernel(core_ref, own_hbm, row_hbm, want_ref, slot_ref, slot_col_ref, own_ref, row_ref, sems):
    copies = [
        pltpu.make_async_copy(own_hbm, own_ref, sems.at[0]),
        pltpu.make_async_copy(row_hbm, row_ref, sems.at[1]),
    ]
    for copy in copies:
        copy.start()
    for copy in copies:
        copy.wait()
    own = own_ref[...]
    own_rows = [
        jnp.concatenate([own[2 * t : 2 * t + 1], own[2 * t + 1 : 2 * t + 2]], axis=1)
        for t in range(TABLES)
    ]
    own_cols = jnp.transpose(jnp.concatenate(own_rows + own_rows, axis=0))
    row_cols = jnp.transpose(jnp.concatenate([row_ref[...], row_ref[...]], axis=0))
    before = iota((IMPS, IMPS), 0) < iota((IMPS, IMPS), 1)
    slots = []
    for t in range(TABLES):
        same = (own_cols[:, t : t + 1] == own_rows[t]) & before
        rank = jnp.sum(jnp.where(same, 1, 0), axis=0, keepdims=True)
        slots.append(own_rows[t] * LINES + (CAP * t) + rank)
    slot_ref[...] = jnp.concatenate(slots, axis=0)
    slot_cols = jnp.transpose(jnp.concatenate(slots + slots, axis=0))
    slot_col_ref[...] = slot_cols
    lines = []
    for t in range(TABLES):
        slot = jnp.broadcast_to(slot_cols[:, t : t + 1], (IMPS, OWNERS))
        row = jnp.broadcast_to(row_cols[:, t : t + 1], (IMPS, OWNERS))
        for r in range(CAP):
            target = iota((IMPS, OWNERS), 1) * LINES + (CAP * t + r)
            lines.append(jnp.sum(jnp.where(slot == target, row, 0), axis=0, keepdims=True))
    want_ref[...] = jnp.transpose(jnp.concatenate(lines, axis=0))


def serve_kernel(req_ref, far_ref, out_ref, wide_ref, tab_ref, sems):
    copies = [pltpu.make_async_copy(far_ref.at[t], tab_ref.at[t], sems.at[t]) for t in range(TABLES)]
    for copy in copies:
        copy.start()
    req = req_ref[...]
    part = ROWS // FOLD
    for t in range(TABLES):
        rows = [req[:, CAP * t + r : CAP * t + r + 1] for r in range(CAP)]
        hot = jnp.concatenate([hot_rows(row & 127, (row >> 7) & 7, 8) for row in rows], axis=0)
        copies[t].wait()
        table = jnp.concatenate(
            [tab_ref[t, f * part : (f + 1) * part, :] for f in range(FOLD)], axis=1
        )
        wide = jnp.dot(hot, table, preferred_element_type=F32)
        for r in range(CAP):
            which = jnp.broadcast_to(rows[r] >> 10, (OWNERS, EMB))
            wide_ref[pl.ds(CAP * t + r, OWNERS, stride=LINES), :] = chosen(
                wide[r * OWNERS : (r + 1) * OWNERS], which
            )
    out_ref[...] = wide_ref[...].astype(BF).reshape(OWNERS, LINES, EMB)


def step_kernel(
    core_ref, ret_ref, slot_col_ref, ses_ref, rel_ref, lb_ref, w_ref, b_ref, ws_ref,
    pre_grad_ref, keep_ref, send_ref, dense_ref,
):
    back = ret_ref[...].reshape(OWNERS * LINES, EMB)
    half = OWNERS * LINES // 2
    source = jnp.concatenate([back[:half], back[half:]], axis=1)
    slot_cols = slot_col_ref[...]
    pieces = []
    for t in range(TABLES):
        slot = slot_cols[:, t : t + 1]
        both = jnp.dot(hot_rows(slot & 127, (slot >> 7) & 7, 8), source, preferred_element_type=F32)
        upper = jnp.broadcast_to(slot, (IMPS, EMB)) >= half
        pieces.append(jnp.where(upper, both[:, EMB:], both[:, :EMB]).astype(BF))
    inputs = jnp.concatenate(pieces, axis=1)
    w_bf = w_ref[...].astype(BF)
    w_score = ws_ref[...]
    pre = jnp.dot(inputs, w_bf, preferred_element_type=F32) + b_ref[...]
    sig = jax.nn.sigmoid(pre)
    hidden = pre * sig
    aux = jnp.transpose(
        jnp.concatenate(
            [rel_ref[...], lb_ref[...], ses_ref[...].astype(F32)] + [rel_ref[...]] * 5, axis=0
        )
    )
    relevance, bias_col, session = aux[:, 0:1], aux[:, 1:2], aux[:, 2:3]
    scores = jnp.sum(hidden * w_score, axis=1, keepdims=True) + bias_col
    first = session < 0.5
    low = jnp.float32(-jnp.inf)
    top = [jnp.max(jnp.where(m, scores, low), axis=0, keepdims=True) for m in (first, ~first)]
    shifted = scores - jnp.where(first, top[0], top[1])
    exponent = jnp.exp(shifted)
    total = [jnp.sum(jnp.where(m, exponent, 0.0), axis=0, keepdims=True) for m in (first, ~first)]
    weight = [jnp.sum(jnp.where(m, relevance, 0.0), axis=0, keepdims=True) for m in (first, ~first)]
    probability = exponent / jnp.where(first, total[0], total[1])
    target = relevance / jnp.where(first, weight[0], weight[1])
    loss = jnp.log(total[0]) + jnp.log(total[1]) - jnp.sum(target * shifted, axis=0, keepdims=True)
    score_grad = probability - target
    pre_grad = score_grad * w_score * (sig * (1.0 + pre * (1.0 - sig)))
    pre_grad_bf = pre_grad.astype(BF)
    pre_grad_ref[...] = pre_grad_bf
    dense_ref[...] = lax.dot_general(
        inputs, pre_grad_bf, (((0,), (0,)), ((), ())), preferred_element_type=F32
    )
    bias_grad = jnp.sum(pre_grad, axis=0, keepdims=True)
    score_w_grad = jnp.sum(score_grad * hidden, axis=0, keepdims=True)
    start = pl.multiple_of(core_ref[0] * 256, 256)
    for q in range(4):
        columns = slice(EMB * q, EMB * (q + 1))
        keep_ref[256 * q : 256 * (q + 1)] = dense_ref[pl.ds(start, 256), columns]
        send_ref[256 * q : 256 * (q + 1)] = dense_ref[pl.ds(256 - start, 256), columns]

    def rows_of(line, last):
        parts = [line[:, EMB * q : EMB * (q + 1)] for q in range(4)]
        return jnp.concatenate(parts + [last] + [jnp.zeros((3, EMB), F32)], axis=0)

    first_core = jnp.broadcast_to(core_ref[0], (8, EMB)) == 0
    for_zero = rows_of(bias_grad, jnp.broadcast_to(loss, (1, EMB)))
    for_one = rows_of(score_w_grad, jnp.zeros((1, EMB), F32))
    keep_ref[1024:] = jnp.where(first_core, for_zero, for_one)
    send_ref[1024:] = jnp.where(first_core, for_one, for_zero)


def back_kernel(pre_grad_ref, slot_ref, slot_col_ref, w_ref, out_ref):
    w_bf = w_ref[...].astype(BF)
    grad = jnp.dot(pre_grad_ref[...], w_bf.T, preferred_element_type=F32).astype(BF).astype(F32)
    slots, slot_cols = slot_ref[...], slot_col_ref[...]
    values, hots = [], []
    for t in range(TABLES):
        which = jnp.broadcast_to(slot_cols[:, t : t + 1] >> 9, (IMPS, EMB))
        values.append(fanned(grad[:, t * EMB : (t + 1) * EMB], which).astype(BF))
        slot = slots[t : t + 1]
        hots.append(hot_cols(slot & 127, (slot >> 7) & 3, 4))
    placed = jnp.dot(
        jnp.concatenate(hots, axis=1), jnp.concatenate(values, axis=0), preferred_element_type=F32
    )
    part = OWNERS // FOLD
    for f in range(FOLD):
        out_ref[f * part : (f + 1) * part] = (
            placed[:, f * EMB : (f + 1) * EMB].astype(BF).reshape(part, LINES, EMB)
        )


def pack_kernel(line_ref, keep_ref, came_ref, out_ref, small_ref, half_ref, sems):
    copies = [
        pltpu.make_async_copy(line_ref, out_ref.at[:, :LINES], sems.at[0]),
        pltpu.make_async_copy(half_ref, out_ref.at[:, LINES:], sems.at[1]),
    ]
    copies[0].start()
    for x in range(4):
        for z in range(8):
            for y in range(4):
                k = 256 * (z % 4) + 16 * (4 * x + y) + 4 * (z // 4)
                half = keep_ref[k : k + 4] + came_ref[k : k + 4]
                high = half.astype(BF).astype(F32)
                half_ref[(x * 8 + z) * 4 + y] = jnp.concatenate([high, half - high], axis=0).astype(BF)
    copies[1].start()
    small_ref[...] = keep_ref[1024:] + came_ref[1024:]
    for copy in copies:
        copy.wait()


def chip_kernel(at_ref, keep_ref, came_ref, own_ref, one_ref, two_ref, three_ref, sum_ref):
    for y in range(4):
        for x in range(4):
            for q in range(4):
                k, to = 256 * q + 16 * (4 * x + y) + 8, 8 * ((y * 4 + x) * 4 + q)
                sum_ref[to : to + 8] = keep_ref[k : k + 8] + came_ref[k : k + 8]
    for d, ref in enumerate((own_ref, one_ref, two_ref, three_ref)):
        ref[...] = sum_ref[pl.ds(pl.multiple_of(((at_ref[0] + d) & 3) * 128, 128), 128), :]


def cross_kernel(
    at_ref, mine_ref, a_ref, b_ref, c_ref, own_ref, one_ref, two_ref, three_ref, sum_ref
):
    sum_ref[...] = (mine_ref[...] + a_ref[...]) + (b_ref[...] + c_ref[...])
    for d, ref in enumerate((own_ref, one_ref, two_ref, three_ref)):
        ref[...] = sum_ref[pl.ds(pl.multiple_of(((at_ref[0] + d) & 3) * 32, 32), 32), :]


def plane_kernel(mine_ref, a_ref, b_ref, c_ref, out_ref):
    out_ref[...] = (mine_ref[...] + a_ref[...]) + (b_ref[...] + c_ref[...])


def lines_kernel(got_ref, id_ref, line_ref):
    line_ref[:OWNERS] = got_ref[:, :LINES]
    ids = jnp.transpose(id_ref[...])
    line_ref[OWNERS] = (ids >> 6).astype(F32).astype(BF)
    line_ref[OWNERS + 1] = (ids & 63).astype(F32).astype(BF)


def open_kernel(got_ref, small_ref, plane_ref, chunk_ref):
    sums = [jnp.zeros((8, EMB), F32) for _ in range(4)]
    for k in range(OWNERS):
        sums[k % 4] = sums[k % 4] + got_ref[k, LINES:].astype(F32)
    total = (sums[0] + sums[1]) + (sums[2] + sums[3])
    half = total[:4] + total[4:]
    last = jnp.concatenate([half, jnp.zeros((4, EMB), F32)], axis=0)
    for k in range(8):
        chunk_ref[k, :32] = plane_ref[...]
        chunk_ref[k, 32:40] = small_ref[...]
        chunk_ref[k, 40:] = last


def column_kernel(got_ref, out_ref, column_ref, sems):
    total = got_ref[0, :40]
    for z in range(1, 8):
        total = total + got_ref[z, :40]
    tiles = [
        jnp.concatenate([got_ref[q, 40:44], got_ref[q + 4, 40:44]], axis=0) for q in range(4)
    ]
    column_ref[...] = jnp.concatenate(tiles + [total], axis=0)
    copies = [pltpu.make_async_copy(column_ref, out_ref.at[p], sems.at[p]) for p in range(16)]
    for copy in copies:
        copy.start()
    for copy in copies:
        copy.wait()


def place_kernel(
    core_ref, own_ref, other_ref, out_ref, wide_ref, buf_ref, sems
):
    core = core_ref[0]
    lines = OWNERS * LINES
    wide_ref[:lines] = own_ref[:OWNERS].reshape(lines, EMB).astype(F32)
    wide_ref[lines:] = other_ref[:OWNERS].reshape(lines, EMB).astype(F32)
    rows = [
        ref[OWNERS].astype(F32).astype(jnp.int32) * 64 + ref[OWNERS + 1].astype(F32).astype(jnp.int32)
        for ref in (own_ref, other_ref)
    ]
    cols = [jnp.transpose(r) for r in rows]
    part = ROWS // 2 // FOLD
    copies = []
    for t in range(TABLES):
        values, hots = [], []
        for s in range(2):
            for r in range(CAP):
                j = CAP * t + r
                line = wide_ref[pl.ds(s * lines + j, OWNERS, stride=LINES), :]
                which = jnp.broadcast_to(cols[s][:, j : j + 1] >> 9, (OWNERS, EMB)) - FOLD * core
                values.append(fanned(line, which).astype(BF))
                row = rows[s][j : j + 1]
                hots.append(hot_cols(row & 127, (row >> 7) & 3, 4))
        total = jnp.dot(
            jnp.concatenate(hots, axis=1), jnp.concatenate(values, axis=0), preferred_element_type=F32
        )
        for f in range(FOLD):
            x = total[:, f * EMB : (f + 1) * EMB]
            mean = jnp.sum(x * x, axis=1, keepdims=True) * (1.0 / EMB)
            buf_ref[t, part * f : part * (f + 1)] = x * (1.0 / (jnp.sqrt(mean) + 1e-06))
        copy = pltpu.make_async_copy(buf_ref.at[t], out_ref.at[t], sems.at[t])
        copy.start()
        copies.append(copy)
    for copy in copies:
        copy.wait()


def squares_of(ref):
    sums = [jnp.zeros((8, EMB), F32) for _ in range(4)]
    for p in range(16):
        for z in range(8):
            tile = ref[p, 8 * z : 8 * (z + 1)]
            sums[z % 4] = sums[z % 4] + tile * tile
    small = ref[0, 64:]
    for p in range(1, 16):
        small = small + ref[p, 64:]
    return (sums[0] + sums[1]) + (sums[2] + sums[3]), small


def square_kernel(own_ref, main_ref, small_ref):
    main_ref[...], small_ref[...] = squares_of(own_ref)


def final_kernel(
    core_ref, own_ref, other_ref, own_main_ref, own_small_ref, w_ref, b_ref, s_ref, loss_ref
):
    start = core_ref[0] * 256
    other_main, other_small = squares_of(other_ref)
    own_small = own_small_ref[...]
    first_core = jnp.broadcast_to(core_ref[0], (8, EMB)) == 0
    bias = jnp.where(first_core, own_small, other_small)
    score = jnp.where(first_core, other_small, own_small)
    square = jnp.sum(bias[0:4] * bias[0:4] + score[0:4] * score[0:4], axis=0, keepdims=True)
    main = own_main_ref[...] + other_main
    square = jnp.sum(square + jnp.sum(main, axis=0, keepdims=True), axis=1, keepdims=True)
    factor = 1.0 / jnp.sqrt(square * (1.0 / (HID * HID + 2 * HID)) + 1e-06)
    for p in range(16):
        for z in range(8):
            row = 8 * (2 * p + z // 4)
            columns = slice(EMB * (z % 4), EMB * (z % 4 + 1))
            w_ref[pl.ds(pl.multiple_of(start + row, 8), 8), columns] = (
                own_ref[p, 8 * z : 8 * (z + 1)] * factor
            )
            w_ref[pl.ds(pl.multiple_of(256 - start + row, 8), 8), columns] = (
                other_ref[p, 8 * z : 8 * (z + 1)] * factor
            )
    b_ref[...] = bias[0:4] * factor
    s_ref[...] = score[0:4] * factor
    loss_ref[...] = bias[4:5] * (1.0 / 512)


def sds(shape, dtype):
    return jax.ShapeDtypeStruct(shape, dtype)


def call(kernel, mib, outs, ins, scratch=(), out_specs=None, flops=1 << 28):
    return pl.pallas_call(
        kernel,
        out_shape=outs,
        in_specs=ins,
        out_specs=(VMEM,) * len(outs) if out_specs is None else out_specs,
        scratch_shapes=list(scratch),
        cost_estimate=pl.CostEstimate(flops=flops, bytes_accessed=1 << 20, transcendentals=0),
        compiler_params=pltpu.CompilerParams(vmem_limit_bytes=mib << 20),
    )


def exchange(array, axes):
    return lax.all_to_all(array, axes, split_axis=0, concat_axis=0, tiled=True)


def whole_step(
    tables, owner_ids, row_ids, session_of, relevance, logit_bias, w_hidden, bias_hidden, w_score
):
    core = lax.axis_index("dp").astype(jnp.int32).reshape(1)
    swap = [(0, 1), (1, 0)]
    i32 = jnp.int32
    wanted, slots, slot_cols = call(
        slots_kernel, 8,
        (sds((OWNERS, LINES), i32), sds((TABLES, IMPS), i32), sds((IMPS, 2 * TABLES), i32)),
        [SMEM, HBM, HBM],
        [pltpu.VMEM((8, 128), i32), pltpu.VMEM((TABLES, IMPS), i32), pltpu.SemaphoreType.DMA((2,))],
    )(
        core,
        pltpu.with_memory_space_constraint(owner_ids.reshape(8, 128), pltpu.HBM),
        pltpu.with_memory_space_constraint(row_ids.reshape(TABLES, IMPS), pltpu.HBM),
    )
    requested = exchange(wanted, TABLE)
    (served,) = call(
        serve_kernel, 24,
        (sds((OWNERS, LINES, EMB), BF),),
        [VMEM, HBM],
        [
            pltpu.VMEM((OWNERS * LINES, EMB), F32),
            pltpu.VMEM((TABLES, ROWS, EMB), BF),
            pltpu.SemaphoreType.DMA((TABLES,)),
        ],
    )(requested, pltpu.with_memory_space_constraint(tables, pltpu.HBM))
    returned = exchange(served, TABLE)
    half = sds((1024 + SMALL, EMB), F32)
    pre_grad, keep, send = call(
        step_kernel, 24,
        (sds((IMPS, HID), BF), half, half),
        [SMEM] + [VMEM] * 8,
        [pltpu.VMEM((HID, HID), F32)],
    )(
        core, returned, slot_cols, session_of, relevance, logit_bias, w_hidden,
        bias_hidden.reshape(1, HID), w_score.reshape(1, HID),
    )
    came = lax.ppermute(send, "dp", swap)
    (lines,) = call(
        back_kernel, 20, (sds((OWNERS, LINES, EMB), BF),), [VMEM] * 4
    )(pre_grad, slots, slot_cols, w_hidden)
    message, small = call(
        pack_kernel, 12,
        (sds((OWNERS, LINES + 8, EMB), BF), sds((SMALL, EMB), F32)),
        [VMEM] * 3,
        [pltpu.VMEM((OWNERS, 8, EMB), BF), pltpu.SemaphoreType.DMA((2,))],
        out_specs=(HBM, VMEM),
    )(lines, keep, came)
    got = exchange(message, TABLE)

    def spread(parts, axis):
        return [
            lax.ppermute(part, axis, [(i, (i + d) % 4) for i in range(4)])
            for d, part in enumerate(parts, 1)
        ]

    quarter, tiles = sds((128, EMB), F32), sds((32, EMB), F32)
    own, *rest = call(
        chip_kernel, 8, (quarter,) * 4, [SMEM] + [VMEM] * 2,
        [pltpu.VMEM((512, EMB), F32)],
    )(lax.axis_index("y").astype(i32).reshape(1), keep, came)
    rest = spread(rest, "y")
    own, *rest = call(
        cross_kernel, 8, (tiles,) * 4, [SMEM] + [VMEM] * 4,
        [pltpu.VMEM((128, EMB), F32)],
    )(lax.axis_index("x").astype(i32).reshape(1), own, *rest)
    rest = spread(rest, "x")
    (plane,) = call(plane_kernel, 8, (tiles,), [VMEM] * 4)(own, *rest)
    (chunks,) = call(open_kernel, 12, (sds((8, 48, EMB), F32),), [VMEM] * 3)(got, small, plane)
    (incoming,) = call(
        lines_kernel, 12, (sds((OWNERS + 2, LINES, EMB), BF),), [VMEM] * 2
    )(got, requested)
    other = lax.ppermute(incoming, "dp", swap)
    column = exchange(chunks, "z")
    (emb_step,) = call(
        place_kernel, 28,
        (sds((TABLES, ROWS // 2, EMB), F32),),
        [SMEM] + [VMEM] * 2,
        [
            pltpu.VMEM((2 * OWNERS * LINES, EMB), F32),
            pltpu.VMEM((TABLES, ROWS // 2, EMB), F32),
            pltpu.SemaphoreType.DMA((TABLES,)),
        ],
        out_specs=(ANY,),
    )(core, incoming, other)
    (sums,) = call(
        column_kernel, 12, (sds((16, 64 + SMALL, EMB), F32),), [VMEM],
        [pltpu.VMEM((64 + SMALL, EMB), F32), pltpu.SemaphoreType.DMA((16,))],
        out_specs=(HBM,),
    )(column)
    mine = exchange(sums, ("x", "y"))
    theirs = lax.ppermute(mine, "dp", swap)
    tile = sds((8, EMB), F32)
    own_main, own_small = call(square_kernel, 8, (tile, tile), [VMEM])(mine)
    step_hidden, step_bias, step_score, loss = call(
        final_kernel, 12,
        (sds((HID, HID), F32), sds((4, 128), F32), sds((4, 128), F32), sds((1, 128), F32)),
        [SMEM] + [VMEM] * 4,
    )(core, mine, theirs, own_main, own_small)
    return emb_step, step_hidden, step_bias.reshape(HID), step_score.reshape(HID), loss[0, 0]


def solution(mesh):
    split = Mesh(mesh.devices.reshape(4, 8, 4, mesh.shape["dp"]), ALL)
    return jax.shard_map(
        whole_step,
        mesh=split,
        in_specs=(
            P(None, TABLE, None),
            P(ALL, None, None, None),
            P(ALL, None, None),
            P(ALL, None),
            P(ALL, None),
            P(ALL, None),
            P(),
            P(),
            P(),
        ),
        out_specs=(P(None, ALL, None), P(), P(), P(), P()),
        check_vma=False,
    )
```
